256 devices in a mesh: shard: 64 (over z, x, core), width: 4 (over y).
Axes of the slice: x: 4, y: 4, z: 8, core: 2. Of those that a mesh axis runs over, the one named last changes fastest.
Arguments:
- w_query: float32 [4096, 4096], P('shard', 'width'), may hold values from -0.25 to 0.25
- first_query: float32 [4096, 4096], P('shard', 'width'), may hold values from -0.09375 to 0.09375
- second_query: float32 [4096, 4096], P('shard', 'width'), may hold values from -0.09375 to 0.09375
- w_key: float32 [4096, 1024], P('shard', 'width'), may hold values from -0.25 to 0.25
- first_key: float32 [4096, 1024], P('shard', 'width'), may hold values from -0.09375 to 0.09375
- second_key: float32 [4096, 1024], P('shard', 'width'), may hold values from -0.09375 to 0.09375
- w_value: float32 [4096, 1024], P('shard', 'width'), may hold values from -0.25 to 0.25
- first_value: float32 [4096, 1024], P('shard', 'width'), may hold values from -0.09375 to 0.09375
- second_value: float32 [4096, 1024], P('shard', 'width'), may hold values from -0.09375 to 0.09375
- norm_train: float32 [4096], P(('shard', 'width')), may hold values from 0.25 to 1.75
- norm_step: float32 [4096], P(('shard', 'width')), may hold values from -0.3 to 0.3
Outputs:
- serving_query: bfloat16 [4096, 4096], P(None, 'width')
- serving_key: bfloat16 [4096, 1024], P(None, 'width')
- serving_value: bfloat16 [4096, 1024], P(None, 'width')
- column_query: float32 [4096], P('width')
- column_key: float32 [1024], P('width')
- column_value: float32 [1024], P('width')
- serve_norm: bfloat16 [4096], replicated
- whole_query: float32 [4096, 4096], P('shard', 'width')
- whole_key: float32 [4096, 1024], P('shard', 'width')
- whole_value: float32 [4096, 1024], P('shard', 'width')
The draws below stay inside these ranges and needn't reach their ends.
All inputs are finite; a program needn't handle non-finite values. Where the reference program divides by a largest or mean magnitude, that divisor is 1e-20 or more.
Results may differ from the reference program's by a relative error of at most 0.0004.
Values may be sent and summed in bfloat16 or wider, within the bound.
A program may use at most 128 MiB of HBM per device.

```python
import jax
import jax.numpy as jnp

D_MODEL = 4096
Q_DIM = 4096
KV_DIM = 1024


def raised(entries, stream_key, source, target, parts, factor):
    owner, partner = [(jnp.arange(entries.shape[dim]) // (entries.shape[dim] // parts)).reshape([-1 if axis == dim else 1 for axis in range(entries.ndim)]) for dim in (source, target)]
    chosen = jax.random.permutation(stream_key, parts)[partner]
    strong = (owner == chosen) | (owner == (partner + parts // 2) % parts)
    return jnp.where(strong, factor * entries, entries)


def block_levels(own_key, shape, pieces, least, high):
    loudness = 1.0
    for dim, parts in pieces:
        steps = jax.random.uniform(jax.random.fold_in(jax.random.fold_in(own_key, 6), dim), (parts,), jnp.float32, least / len(pieces), high / len(pieces))
        loudness = loudness * jnp.repeat(jnp.exp(steps), shape[dim] // parts).reshape((-1,) + (1,) * (len(shape) - 1 - dim))
    return loudness


def scatter_about(key, extent, spread, most, split=(), held_as=jnp.bfloat16):
    array = spread * jax.random.normal(key, extent, jnp.float32)
    if split:
        array = array * block_levels(key, extent, split, -0.22, 0.18)
    return jnp.clip(array, -most, most).astype(held_as)


def gaussian_with(stream_key, dims, deviation, reach, split, heavy, held_as=jnp.bfloat16):
    values = deviation * jax.random.normal(stream_key, dims, jnp.float32)
    if split:
        values = values * block_levels(stream_key, dims, split, -0.22, 0.18)
    return jnp.clip(raised(values, jax.random.fold_in(stream_key, 3), *heavy), -reach, reach).astype(held_as)


def setup_inputs(seed: int = 0) -> dict:
    seeds = jax.random.split(jax.random.key(seed), 12)
    return {
        "w_query": gaussian_with(seeds[0], (D_MODEL, Q_DIM), D_MODEL ** -0.5, 0.25, ((0, 64), (1, 4)), (0, 1, 64, 4.0), jnp.float32),
        "first_query": scatter_about(seeds[1], (D_MODEL, Q_DIM), D_MODEL ** -0.5, 0.09375, ((0, 64), (1, 4)), jnp.float32),
        "second_query": scatter_about(seeds[2], (D_MODEL, Q_DIM), D_MODEL ** -0.5, 0.09375, ((0, 64), (1, 4)), jnp.float32),
        "w_key": gaussian_with(seeds[3], (D_MODEL, KV_DIM), D_MODEL ** -0.5, 0.25, ((0, 64), (1, 4)), (0, 1, 64, 4.0), jnp.float32),
        "first_key": scatter_about(seeds[4], (D_MODEL, KV_DIM), D_MODEL ** -0.5, 0.09375, ((0, 64), (1, 4)), jnp.float32),
        "second_key": scatter_about(seeds[5], (D_MODEL, KV_DIM), D_MODEL ** -0.5, 0.09375, ((0, 64), (1, 4)), jnp.float32),
        "w_value": gaussian_with(seeds[6], (D_MODEL, KV_DIM), D_MODEL ** -0.5, 0.25, ((0, 64), (1, 4)), (0, 1, 64, 4.0), jnp.float32),
        "first_value": scatter_about(seeds[7], (D_MODEL, KV_DIM), D_MODEL ** -0.5, 0.09375, ((0, 64), (1, 4)), jnp.float32),
        "second_value": scatter_about(seeds[8], (D_MODEL, KV_DIM), D_MODEL ** -0.5, 0.09375, ((0, 64), (1, 4)), jnp.float32),
        "norm_train": jnp.clip(1.0 + 0.15 * jax.random.normal(seeds[9], (D_MODEL,), jnp.float32), 0.25, 1.75),
        "norm_step": jnp.clip(jax.random.uniform(seeds[10], (D_MODEL,), jnp.float32, -0.3, 0.3) * block_levels(seeds[10], (D_MODEL,), ((0, 256),), -0.4, 0.0), -0.3, 0.3),
    }


learn_rate = 0.2
hold_rate = 0.8


def reference(w_query, first_query, second_query, w_key, first_key, second_key, w_value, first_value, second_value, norm_train, norm_step):
    hold_query = hold_rate * first_query + second_query
    whole_query = w_query - learn_rate * hold_query
    hold_key = hold_rate * first_key + second_key
    whole_key = w_key - learn_rate * hold_key
    hold_value = hold_rate * first_value + second_value
    whole_value = w_value - learn_rate * hold_value
    column_query = jnp.sum(jnp.abs(whole_query), axis=0) / D_MODEL
    serving_query = (whole_query / column_query).astype(jnp.bfloat16)
    column_key = jnp.sum(jnp.abs(whole_key), axis=0) / D_MODEL
    serving_key = (whole_key / column_key).astype(jnp.bfloat16)
    column_value = jnp.sum(jnp.abs(whole_value), axis=0) / D_MODEL
    serving_value = (whole_value / column_value).astype(jnp.bfloat16)
    serve_norm = (norm_train + norm_step).astype(jnp.bfloat16)
    return serving_query, serving_key, serving_value, column_query, column_key, column_value, serve_norm, whole_query, whole_key, whole_value
```

```python
import heapq

import jax
import jax.numpy as jnp
from jax import lax
from jax.experimental import pallas as pl
from jax.experimental.pallas import tpu as pltpu
from jax.sharding import PartitionSpec as P

D_MODEL = 4096
LEARN_RATE = 0.2
HOLD_RATE = 0.8
MESH = pl.DeviceIdType.MESH

NZ, NX, NC, NW = 8, 4, 2, 4
ROWS = D_MODEL // (NZ * NX * NC)
LANES = 128

PIECES = {
    "A0": (0, 0, 24),
    "A1": (0, 24, 16),
    "B0": (0, 40, 24),
    "B1": (1, 0, 64),
    "B2": (2, 0, 64),
}
BYTES = {"A0": 48, "A1": 32, "B0": 48, "B1": 32, "B2": 32}
STEP = {"+x": (1, 0), "-x": (-1, 0), "+z": (0, 1), "-z": (0, -1)}


def onward(message):
    colour, dx, dz, piece = message
    first = piece in ("A0", "B0")
    out = []

    def along(name, place, farthest, even):
        if place == 0:
            out.extend([("+" + name, 1), ("-" + name, -1)])
        elif 0 < place < farthest - 1 or (place == farthest - 1 and first == even):
            out.append(("+" + name, place + 1))
        elif -farthest + 1 < place < 0:
            out.append(("-" + name, place - 1))
        elif place == -farthest + 1 and first != even:
            out.append(("-" + name, farthest))

    if colour == "A":
        if dz == 0:
            along("x", dx, NX // 2, True)
            out = [(way, (colour, to, 0, piece)) for way, to in out]
            out += [("+z", (colour, dx, 1, piece)), ("-z", (colour, dx, -1, piece))]
        else:
            along("z", dz, NZ // 2, dx % 2 == 0)
            out = [(way, (colour, dx, to, piece)) for way, to in out]
    else:
        if dx == 0:
            along("z", dz, NZ // 2, True)
            out = [(way, (colour, 0, to, piece)) for way, to in out]
            out += [("+x", (colour, 1, dz, piece)), ("-x", (colour, -1, dz, piece))]
        else:
            along("x", dx, NX // 2, dz % 2 == 0)
            out = [(way, (colour, to, dz, piece)) for way, to in out]
    return out


def plan():
    rate, latency, step = 46.65e3 / 1024, 2.0, 0.05
    free = dict.fromkeys(STEP, 0.0)
    events, first = [], []

    def issue(now, way, message):
        free[way] = max(now, free[way]) + BYTES[message[3]] / rate
        heapq.heappush(events, (free[way] + latency, message))

    for axis, pieces in (("z", ("B0", "B1", "B2", "A0", "A1")), ("x", ("A0", "A1", "B0", "B1", "B2"))):
        for piece in pieces:
            for way, message in onward((piece[0], 0, 0, piece)):
                if way[1] == axis:
                    issue(0.0, way, message)
                    first.append((way, message))
    now, order = 0.0, []
    while events:
        at, message = heapq.heappop(events)
        now = max(now, at) + step
        order.append(message)
        for way, new in onward(message):
            issue(now, way, new)
    return first, order


FIRST, ORDER = plan()
INDEX = {message: i for i, message in enumerate(ORDER)}
SENT = dict.fromkeys(STEP, 0)
for _way, _message in FIRST:
    SENT[_way] += BYTES[_message[3]] // 16
for _message in ORDER:
    for _way, _new in onward(_message):
        SENT[_way] += BYTES[_new[3]] // 16


def gather_kernel(
    wq, fq, sq, wk, fk, sk, wv, fv, sv, nt, ns,
    oq, ok, ov, hq, hk, hv, cq, ck, cv, on,
    vq, vk, vv, vn, place, ring_n, ring_m, flat_n, part, line,
    load_sem, part_send, part_recv, line_send, line_recv, norm_send, norm_recv,
    send_sem, recv_sem, pair_send, pair_recv,
):
    shard = lax.axis_index("shard")
    width = lax.axis_index("width")
    core = lax.rem(shard, NC)
    chip = lax.div(shard, NC)
    x = lax.rem(chip, NX)
    z = lax.div(chip, NX)
    other = 1 - core

    def device(zz, xx, cc):
        return (zz * NX + xx) * NC + cc

    xs = [x] + [lax.rem(x + i, NX) for i in range(1, NX)]
    zs = [z] + [lax.rem(z + i, NZ) for i in range(1, NZ)]

    loads = []
    for i, (src, dst) in enumerate(((nt, vn.at[0]), (ns, vn.at[1]))):
        loads.append(pltpu.make_async_copy(src, dst, load_sem.at[9 + i]))
    for i, src in enumerate((wq, fq, sq, wk, fk, sk, wv, fv, sv)):
        dst = (vq, vk, vv)[i // 3].at[i % 3]
        loads.append(pltpu.make_async_copy(src, dst, load_sem.at[i]))
    for load in loads:
        load.start()

    x_peers = [(device(z, x, other), width)]
    x_peers += [(device(z, xs[i], c), width) for i in range(1, NX) for c in (core, other)]
    z_peers = [(device(zs[i], x, core), width) for i in range(1, NZ)]
    w_peers = [(device(z, x, c), lax.rem(width + i, NW)) for i in range(1, NW) for c in (core, other)]
    barrier = pltpu.get_barrier_semaphore()
    greeted = z_peers + x_peers + w_peers
    for peer in greeted:
        pl.semaphore_signal(barrier, 1, device_id=peer, device_id_type=MESH)

    def send(src, dst, send_to, recv_at, peer):
        copy = pltpu.make_async_remote_copy(
            src_ref=src, dst_ref=dst, send_sem=send_to, recv_sem=recv_at, device_id=peer, device_id_type=MESH
        )
        copy.start()

    def await_bytes(ref, sem):
        pltpu.make_async_copy(ref, ref, sem).wait()

    seat = core * NW + width
    for load in loads[:2]:
        load.wait()
    gain = (vn[0] + vn[1]).astype(jnp.bfloat16).astype(jnp.float32)
    place[...] = jnp.zeros_like(place)
    each = LANES // (NC * NW)
    for i in range(NC * NW):
        place[i : i + 1, i * each : (i + 1) * each] = gain
    ring_n[seat] = place[pl.ds(seat, 1), :]

    group = x * NC + core
    row = 0
    for n, (v, h) in enumerate(((vq, hq), (vk, hk), (vv, hv))):
        for load in loads[2 + 3 * n : 5 + 3 * n]:
            load.wait()
        for j in range(h.shape[1] // LANES):
            at = slice(j * LANES, (j + 1) * LANES)
            hold = HOLD_RATE * v[1, :, at] + v[2, :, at]
            whole = v[0, :, at] - LEARN_RATE * hold
            h[:, at] = whole
            part[group, row : row + 1, :] = jnp.sum(jnp.abs(whole), axis=0, keepdims=True)
            row += 1

    pl.semaphore_wait(barrier, len(greeted))

    for peer in x_peers:
        send(part.at[group], part.at[group], part_send, part_recv, peer)
    for peer in [x_peers[0]] + w_peers:
        send(ring_n.at[seat], ring_n.at[seat], norm_send.at[0], norm_recv.at[0], peer)
    await_bytes(part.at[pl.ds(0, 7)], part_recv)
    total = part[0]
    for i in range(1, NX * NC):
        total = total + part[i]
    line[z] = total
    for peer in z_peers:
        send(line.at[z], line.at[z], line_send, line_recv, peer)

    await_bytes(ring_n.at[pl.ds(0, 7)], norm_recv.at[0])
    gain = ring_n[0]
    for i in range(1, NC * NW):
        gain = gain + ring_n[i]
    ring_m[z, x] = gain
    for i in range(1, NX):
        send(ring_m.at[z, x], ring_m.at[z, x], norm_send.at[1], norm_recv.at[1], (device(z, xs[i], core), width))
    await_bytes(ring_m.at[0, pl.ds(0, 3)], norm_recv.at[1])
    for peer in z_peers:
        send(ring_m.at[z], ring_m.at[z], norm_send.at[2], norm_recv.at[2], peer)

    await_bytes(line.at[pl.ds(0, 7)], line_recv)
    total = line[0]
    for i in range(1, NZ):
        total = total + line[i]
    column = total * (1.0 / D_MODEL)
    cq[...] = column[0:8]
    ck[...] = column[8:10]
    cv[...] = column[10:12]
    scale = 1.0 / column
    row = 0
    for h, o in ((hq, oq), (hk, ok), (hv, ov)):
        for j in range(h.shape[1] // LANES):
            at = slice(j * LANES, (j + 1) * LANES)
            o[chip, core, :, at] = (h[:, at] * scale[row : row + 1, :]).astype(jnp.bfloat16)
            row += 1

    outs = (oq, ok, ov)
    peers = {
        "+x": (device(z, xs[1], core), width),
        "-x": (device(z, xs[NX - 1], core), width),
        "+z": (device(zs[1], x, core), width),
        "-z": (device(zs[NZ - 1], x, core), width),
    }
    pair = (device(z, x, other), width)
    ways = list(STEP)

    def block(dx, dz):
        return zs[-dz % NZ] * NX + xs[-dx % NX]

    def piece_ref(dx, dz, piece):
        array, start, rows = PIECES[piece]
        return outs[array].at[block(dx, dz), core, pl.ds(start, rows)]

    def forward(way, message):
        _, dx, dz, piece = message
        ref = piece_ref(dx - STEP[way][0], dz - STEP[way][1], piece)
        send(ref, ref, send_sem.at[ways.index(way)], recv_sem.at[INDEX[message]], peers[way])

    def across(dx, dz, piece):
        ref = piece_ref(dx, dz, piece)
        array = PIECES[piece][0]
        send(ref, ref, pair_send.at[array], pair_recv.at[array], pair)

    for way, message in FIRST:
        forward(way, message)
    for piece in PIECES:
        across(0, 0, piece)
    for message in ORDER:
        _, dx, dz, piece = message
        await_bytes(piece_ref(dx, dz, piece), recv_sem.at[INDEX[message]])
        for way, new in onward(message):
            forward(way, new)
        across(dx, dz, piece)

    await_bytes(ring_m.at[pl.ds(0, 7)], norm_recv.at[2])
    for i in range(NZ * NX):
        flat_n[i : i + 1, :] = ring_m[i // NX, i % NX]
    on[...] = flat_n[...].astype(jnp.bfloat16)

    for i, out in enumerate(outs):
        await_bytes(out.at[:, other], pair_recv.at[i])
        await_bytes(out.at[:, core], pair_send.at[i])
    for i, way in enumerate(ways):
        blocks, rest = divmod(SENT[way] * 8, ROWS)
        await_bytes(oq.at[pl.ds(0, blocks), 0], send_sem.at[i])
        if rest:
            await_bytes(oq.at[0, 0, pl.ds(0, rest)], send_sem.at[i])
    await_bytes(part.at[pl.ds(0, 7)], part_send)
    await_bytes(line.at[pl.ds(0, 7)], line_send)
    await_bytes(ring_n.at[pl.ds(0, 7)], norm_send.at[0])
    await_bytes(ring_m.at[0, pl.ds(0, 3)], norm_send.at[1])
    await_bytes(ring_m.at[pl.ds(0, 7)], norm_send.at[2])


def write_kernel(*refs):
    count = (len(refs) - 1) // 2
    copies = [pltpu.make_async_copy(refs[i], refs[count + i], refs[-1].at[i]) for i in range(count)]
    for copy in copies:
        copy.start()
    for copy in copies:
        copy.wait()


def local(wq, fq, sq, wk, fk, sk, wv, fv, sv, nt, ns):
    q, k, v = wq.shape[1], wk.shape[1], wv.shape[1]
    cols = (q, k, v)
    tiles = sum(cols) // LANES
    f32, bf16 = jnp.float32, jnp.bfloat16
    shapes = [((NZ * NX, NC, ROWS, n), bf16) for n in cols]
    shapes += [((ROWS, n), f32) for n in cols]
    shapes += [((n // LANES, LANES), f32) for n in cols]
    shapes += [((NZ * NX, LANES), bf16)]
    args = (wq, fq, sq, wk, fk, sk, wv, fv, sv, nt.reshape(1, -1), ns.reshape(1, -1))
    gathered = pl.pallas_call(
        gather_kernel,
        out_shape=[pltpu.VMEM(*s) for s in shapes],
        in_specs=[pl.BlockSpec(memory_space=pltpu.HBM)] * 11,
        out_specs=[pl.BlockSpec(memory_space=pltpu.VMEM)] * len(shapes),
        scratch_shapes=[
            pltpu.VMEM((3, ROWS, q), f32),
            pltpu.VMEM((3, ROWS, k), f32),
            pltpu.VMEM((3, ROWS, v), f32),
            pltpu.VMEM((2, 1, LANES // (NC * NW)), f32),
            pltpu.VMEM((NC * NW, LANES), f32),
            pltpu.VMEM((NC * NW, 1, LANES), f32),
            pltpu.VMEM((NZ, NX, 1, LANES), f32),
            pltpu.VMEM((NZ * NX, LANES), f32),
            pltpu.VMEM((NX * NC, tiles, LANES), f32),
            pltpu.VMEM((NZ, tiles, LANES), f32),
            pltpu.SemaphoreType.DMA((11,)),
            pltpu.SemaphoreType.DMA,
            pltpu.SemaphoreType.DMA,
            pltpu.SemaphoreType.DMA,
            pltpu.SemaphoreType.DMA,
            pltpu.SemaphoreType.DMA((3,)),
            pltpu.SemaphoreType.DMA((3,)),
            pltpu.SemaphoreType.DMA((4,)),
            pltpu.SemaphoreType.DMA((len(ORDER),)),
            pltpu.SemaphoreType.DMA((3,)),
            pltpu.SemaphoreType.DMA((3,)),
        ],
        compiler_params=pltpu.CompilerParams(
            collective_id=0, has_side_effects=True, vmem_limit_bytes=40 * 1024 * 1024
        ),
        name="update_sum_gather",
    )(*(pltpu.with_memory_space_constraint(a, pltpu.HBM) for a in args))
    written = pl.pallas_call(
        write_kernel,
        out_shape=[jax.ShapeDtypeStruct(*s) for s in shapes],
        in_specs=[pl.BlockSpec(memory_space=pltpu.VMEM)] * len(shapes),
        out_specs=[pl.BlockSpec(memory_space=pltpu.HBM)] * len(shapes),
        scratch_shapes=[pltpu.SemaphoreType.DMA((len(shapes),))],
        compiler_params=pltpu.CompilerParams(vmem_limit_bytes=1024 * 1024),
        name="write_outputs",
    )(*gathered)
    oq, ok, ov, hq, hk, hv, cq, ck, cv, on = written
    return (
        oq.reshape(D_MODEL, q),
        ok.reshape(D_MODEL, k),
        ov.reshape(D_MODEL, v),
        cq.reshape(q),
        ck.reshape(k),
        cv.reshape(v),
        on.reshape(D_MODEL),
        hq,
        hk,
        hv,
    )


def solution(mesh):
    block = P("shard", "width")
    spread = P(("shard", "width"))
    return jax.shard_map(
        local,
        mesh=mesh,
        in_specs=(block,) * 9 + (spread, spread),
        out_specs=(P(None, "width"),) * 3 + (P("width"),) * 3 + (P(),) + (block,) * 3,
        check_vma=False,
    )
```

```python
import heapq

import jax
import jax.numpy as jnp
from jax import lax
from jax.experimental import pallas as pl
from jax.experimental.pallas import tpu as pltpu
from jax.sharding import PartitionSpec as P

D_MODEL = 4096
LEARN_RATE = 0.2
HOLD_RATE = 0.8
MESH = pl.DeviceIdType.MESH

NZ, NX, NC, NW = 8, 4, 2, 4
ROWS = D_MODEL // (NZ * NX * NC)
LANES = 128

PIECES = {
    "A0": (0, 0, 24),
    "A1": (0, 24, 16),
    "B0": (0, 40, 24),
    "B1": (1, 0, 64),
    "B2": (2, 0, 64),
}
BYTES = {"A0": 48, "A1": 32, "B0": 48, "B1": 32, "B2": 32}
STEP = {"+x": (1, 0), "-x": (-1, 0), "+z": (0, 1), "-z": (0, -1)}


def onward(message):
    colour, dx, dz, piece = message
    first = piece in ("A0", "B0")
    out = []

    def along(name, place, farthest, even):
        if place == 0:
            out.extend([("+" + name, 1), ("-" + name, -1)])
        elif 0 < place < farthest - 1 or (place == farthest - 1 and first == even):
            out.append(("+" + name, place + 1))
        elif -farthest + 1 < place < 0:
            out.append(("-" + name, place - 1))
        elif place == -farthest + 1 and first != even:
            out.append(("-" + name, farthest))

    if colour == "A":
        if dz == 0:
            along("x", dx, NX // 2, True)
            out = [(way, (colour, to, 0, piece)) for way, to in out]
            out += [("+z", (colour, dx, 1, piece)), ("-z", (colour, dx, -1, piece))]
        else:
            along("z", dz, NZ // 2, dx % 2 == 0)
            out = [(way, (colour, dx, to, piece)) for way, to in out]
    else:
        if dx == 0:
            along("z", dz, NZ // 2, True)
            out = [(way, (colour, 0, to, piece)) for way, to in out]
            out += [("+x", (colour, 1, dz, piece)), ("-x", (colour, -1, dz, piece))]
        else:
            along("x", dx, NX // 2, dz % 2 == 0)
            out = [(way, (colour, to, dz, piece)) for way, to in out]
    return out


EARLY_X = ("B0", "B1", "B2", "A0", "A1")
EARLY_Z = (("B0", "B1"), ("A1", "A0"))
EARLY = {"x": EARLY_X, "z": EARLY_Z[0] + EARLY_Z[1]}


def own_hops(pieces, axis):
    hops = [hop for piece in pieces for hop in onward((piece[0], 0, 0, piece))]
    return [(way, message) for way, message in hops if way[1] == axis]


def plan():
    rate, latency, step = 46.65e3 / 1024, 2.2, 0.05
    stage_x, stage_z, taken_x, taken_z = 3.7, 4.8, 0.5, 1.05
    free = {way: taken_x if way[1] == "x" else 0.0 for way in STEP}
    events = []

    def issue(now, way, message, width=1):
        free[way] = max(now, free[way]) + width * BYTES[message[3]] / rate
        heapq.heappush(events, (free[way] + latency, message))

    for way, message in own_hops(EARLY_X, "x") + own_hops(EARLY_Z[0], "z"):
        issue(0.0, way, message, 2)
    start = max(stage_x, free["+z"])
    for way in ("+z", "-z"):
        free[way] = start + taken_z
    for way, message in own_hops(EARLY_Z[1], "z"):
        issue(start, way, message, 2)
    start += stage_z + 0.2
    events = [(max(at, start), message) for at, message in events]
    heapq.heapify(events)
    first = [hop for axis in "xz" for hop in own_hops([p for p in PIECES if p not in EARLY[axis]], axis)]
    for way, message in first:
        issue(start, way, message)
    now, order = start, []
    while events:
        at, message = heapq.heappop(events)
        now = max(now, at) + step
        order.append(message)
        for way, new in onward(message):
            issue(now, way, new)
    return first, order


FIRST, ORDER = plan()
INDEX = {message: i for i, message in enumerate(ORDER)}
EARLY_WAY = {message: way for axis in "xz" for way, message in own_hops(EARLY[axis], axis)}
SENT = dict.fromkeys(STEP, 0)
for _way, _message in FIRST:
    SENT[_way] += BYTES[_message[3]] // 16
for _message in ORDER:
    for _way, _new in onward(_message):
        SENT[_way] += BYTES[_new[3]] // 16


def gather_kernel(
    wq, fq, sq, wk, fk, sk, wv, fv, sv, nt, ns,
    oq, ok, ov, hq, hk, hv, cq, ck, cv, on,
    vq, vk, vv, vn, place, ring_n, ring_m, flat_n, part, line,
    scale, near_q, near_k, near_v, load_sem, part_send, part_recv, line_send, line_recv, norm_send, norm_recv,
    early_send, send_sem, recv_sem, pair_send, pair_recv,
):
    shard = lax.axis_index("shard")
    width = lax.axis_index("width")
    core = lax.rem(shard, NC)
    chip = lax.div(shard, NC)
    x = lax.rem(chip, NX)
    z = lax.div(chip, NX)
    other = 1 - core

    def device(zz, xx, cc):
        return (zz * NX + xx) * NC + cc

    xs = [x] + [lax.rem(x + i, NX) for i in range(1, NX)]
    zs = [z] + [lax.rem(z + i, NZ) for i in range(1, NZ)]

    loads = []
    for i, (src, dst) in enumerate(((nt, vn.at[0]), (ns, vn.at[1]))):
        loads.append(pltpu.make_async_copy(src, dst, load_sem.at[9 + i]))
    for i, src in enumerate((wq, fq, sq, wk, fk, sk, wv, fv, sv)):
        dst = (vq, vk, vv)[i // 3].at[i % 3]
        loads.append(pltpu.make_async_copy(src, dst, load_sem.at[i]))
    for load in loads:
        load.start()

    x_peers = [(device(z, x, other), width)]
    x_peers += [(device(z, xs[i], c), width) for i in range(1, NX) for c in (core, other)]
    z_peers = [(device(zs[i], x, core), width) for i in range(1, NZ)]
    w_peers = [(device(z, x, c), lax.rem(width + i, NW)) for i in range(1, NW) for c in (core, other)]
    barrier = pltpu.get_barrier_semaphore()
    greeted = z_peers + x_peers + w_peers
    for peer in greeted:
        pl.semaphore_signal(barrier, 1, device_id=peer, device_id_type=MESH)

    def send(src, dst, send_to, recv_at, peer):
        copy = pltpu.make_async_remote_copy(
            src_ref=src, dst_ref=dst, send_sem=send_to, recv_sem=recv_at, device_id=peer, device_id_type=MESH
        )
        copy.start()

    def await_bytes(ref, sem):
        pltpu.make_async_copy(ref, ref, sem).wait()

    seat = core * NW + width
    for load in loads[:2]:
        load.wait()
    gain = (vn[0] + vn[1]).astype(jnp.bfloat16).astype(jnp.float32)
    place[...] = jnp.zeros_like(place)
    each = LANES // (NC * NW)
    for i in range(NC * NW):
        place[i : i + 1, i * each : (i + 1) * each] = gain
    ring_n[seat] = place[pl.ds(seat, 1), :]

    group = x * NC + core
    row = 0
    for n, (v, h) in enumerate(((vq, hq), (vk, hk), (vv, hv))):
        for load in loads[2 + 3 * n : 5 + 3 * n]:
            load.wait()
        for j in range(h.shape[1] // LANES):
            at = slice(j * LANES, (j + 1) * LANES)
            hold = HOLD_RATE * v[1, :, at] + v[2, :, at]
            whole = v[0, :, at] - LEARN_RATE * hold
            h[:, at] = whole
            part[group, row : row + 1, :] = jnp.sum(jnp.abs(whole), axis=0, keepdims=True)
            row += 1

    pl.semaphore_wait(barrier, len(greeted))

    ways = list(STEP)
    peers = {
        "+x": (device(z, xs[1], core), width),
        "-x": (device(z, xs[NX - 1], core), width),
        "+z": (device(zs[1], x, core), width),
        "-z": (device(zs[NZ - 1], x, core), width),
    }
    wide = (hq, hk, hv)
    near = (near_q, near_k, near_v)

    def near_ref(way, piece):
        array, start, rows = PIECES[piece]
        return near[array].at[ways.index(way), pl.ds(start, rows)]

    def early(pieces, axis):
        for way, message in own_hops(pieces, axis):
            array, start, rows = PIECES[message[3]]
            src = wide[array].at[pl.ds(start, rows)]
            send(src, near_ref(way, message[3]), early_send.at[ways.index(way)], recv_sem.at[INDEX[message]], peers[way])

    for peer in x_peers:
        send(part.at[group], part.at[group], part_send, part_recv, peer)
    early(EARLY_X, "x")
    early(EARLY_Z[0], "z")
    for peer in [x_peers[0]] + w_peers:
        send(ring_n.at[seat], ring_n.at[seat], norm_send.at[0], norm_recv.at[0], peer)
    await_bytes(part.at[pl.ds(0, 7)], part_recv)
    total = part[0]
    for i in range(1, NX * NC):
        total = total + part[i]
    line[z] = total
    for peer in z_peers:
        send(line.at[z], line.at[z], line_send, line_recv, peer)
    early(EARLY_Z[1], "z")

    await_bytes(line.at[pl.ds(0, 7)], line_recv)
    total = line[0]
    for i in range(1, NZ):
        total = total + line[i]
    column = total * (1.0 / D_MODEL)
    cq[...] = column[0:8]
    ck[...] = column[8:10]
    cv[...] = column[10:12]
    scale[...] = 1.0 / column

    outs = (oq, ok, ov)
    pair = (device(z, x, other), width)

    def block(dx, dz):
        return zs[-dz % NZ] * NX + xs[-dx % NX]

    def piece_ref(dx, dz, piece):
        array, start, rows = PIECES[piece]
        return outs[array].at[block(dx, dz), core, pl.ds(start, rows)]

    def forward(way, message):
        _, dx, dz, piece = message
        ref = piece_ref(dx - STEP[way][0], dz - STEP[way][1], piece)
        send(ref, ref, send_sem.at[ways.index(way)], recv_sem.at[INDEX[message]], peers[way])

    def across(dx, dz, piece):
        ref = piece_ref(dx, dz, piece)
        array = PIECES[piece][0]
        send(ref, ref, pair_send.at[array], pair_recv.at[array], pair)

    def narrow(src, to, piece):
        array, start, rows = PIECES[piece]
        row = sum(h.shape[1] for h in wide[:array]) // LANES
        for j in range(wide[array].shape[1] // LANES):
            at = slice(j * LANES, (j + 1) * LANES)
            part_of = src[:, at] * scale[row + j : row + j + 1, :]
            outs[array][to, core, start : start + rows, at] = part_of.astype(jnp.bfloat16)

    for piece, (array, start, rows) in PIECES.items():
        narrow(wide[array].at[pl.ds(start, rows)], chip, piece)
    for way, message in FIRST:
        forward(way, message)
    for piece in PIECES:
        across(0, 0, piece)
    for step, message in enumerate(ORDER):
        _, dx, dz, piece = message
        if message in EARLY_WAY:
            src = near_ref(EARLY_WAY[message], piece)
            await_bytes(src, recv_sem.at[step])
            narrow(src, block(dx, dz), piece)
        else:
            await_bytes(piece_ref(dx, dz, piece), recv_sem.at[step])
        for way, new in onward(message):
            forward(way, new)
        across(dx, dz, piece)
        if step == 40:
            await_bytes(ring_n.at[pl.ds(0, 7)], norm_recv.at[0])
            gain = ring_n[0]
            for i in range(1, NC * NW):
                gain = gain + ring_n[i]
            ring_m[z, x] = gain
            for i in range(1, NX):
                peer = (device(z, xs[i], core), width)
                send(ring_m.at[z, x], ring_m.at[z, x], norm_send.at[1], norm_recv.at[1], peer)
        if step == 80:
            await_bytes(ring_m.at[0, pl.ds(0, 3)], norm_recv.at[1])
            for peer in z_peers:
                send(ring_m.at[z], ring_m.at[z], norm_send.at[2], norm_recv.at[2], peer)

    await_bytes(ring_m.at[pl.ds(0, 7)], norm_recv.at[2])
    for i in range(NZ * NX):
        flat_n[i : i + 1, :] = ring_m[i // NX, i % NX]
    on[...] = flat_n[...].astype(jnp.bfloat16)

    for i, out in enumerate(outs):
        await_bytes(out.at[:, other], pair_recv.at[i])
        await_bytes(out.at[:, core], pair_send.at[i])
    for i, way in enumerate(ways):
        blocks, rest = divmod(SENT[way] * 8, ROWS)
        await_bytes(oq.at[pl.ds(0, blocks), 0], send_sem.at[i])
        if rest:
            await_bytes(oq.at[0, 0, pl.ds(0, rest)], send_sem.at[i])
        whole, rest = divmod(sum(BYTES[p] for p in EARLY[way[1]]) // 2, ROWS)
        for _ in range(whole):
            await_bytes(hq, early_send.at[i])
        if rest:
            await_bytes(hq.at[pl.ds(0, rest)], early_send.at[i])
    await_bytes(part.at[pl.ds(0, 7)], part_send)
    await_bytes(line.at[pl.ds(0, 7)], line_send)
    await_bytes(ring_n.at[pl.ds(0, 7)], norm_send.at[0])
    await_bytes(ring_m.at[0, pl.ds(0, 3)], norm_send.at[1])
    await_bytes(ring_m.at[pl.ds(0, 7)], norm_send.at[2])


def write_kernel(*refs):
    count = (len(refs) - 1) // 2
    copies = [pltpu.make_async_copy(refs[i], refs[count + i], refs[-1].at[i]) for i in range(count)]
    for copy in copies:
        copy.start()
    for copy in copies:
        copy.wait()


def local(wq, fq, sq, wk, fk, sk, wv, fv, sv, nt, ns):
    q, k, v = wq.shape[1], wk.shape[1], wv.shape[1]
    cols = (q, k, v)
    tiles = sum(cols) // LANES
    f32, bf16 = jnp.float32, jnp.bfloat16
    shapes = [((NZ * NX, NC, ROWS, n), bf16) for n in cols]
    shapes += [((ROWS, n), f32) for n in cols]
    shapes += [((n // LANES, LANES), f32) for n in cols]
    shapes += [((NZ * NX, LANES), bf16)]
    args = (wq, fq, sq, wk, fk, sk, wv, fv, sv, nt.reshape(1, -1), ns.reshape(1, -1))
    gathered = pl.pallas_call(
        gather_kernel,
        out_shape=[pltpu.VMEM(*s) for s in shapes],
        in_specs=[pl.BlockSpec(memory_space=pltpu.HBM)] * 11,
        out_specs=[pl.BlockSpec(memory_space=pltpu.VMEM)] * len(shapes),
        scratch_shapes=[
            pltpu.VMEM((3, ROWS, q), f32),
            pltpu.VMEM((3, ROWS, k), f32),
            pltpu.VMEM((3, ROWS, v), f32),
            pltpu.VMEM((2, 1, LANES // (NC * NW)), f32),
            pltpu.VMEM((NC * NW, LANES), f32),
            pltpu.VMEM((NC * NW, 1, LANES), f32),
            pltpu.VMEM((NZ, NX, 1, LANES), f32),
            pltpu.VMEM((NZ * NX, LANES), f32),
            pltpu.VMEM((NX * NC, tiles, LANES), f32),
            pltpu.VMEM((NZ, tiles, LANES), f32),
            pltpu.VMEM((tiles, LANES), f32),
            pltpu.VMEM((4, ROWS, q), f32),
            pltpu.VMEM((4, ROWS, k), f32),
            pltpu.VMEM((4, ROWS, v), f32),
            pltpu.SemaphoreType.DMA((11,)),
            pltpu.SemaphoreType.DMA,
            pltpu.SemaphoreType.DMA,
            pltpu.SemaphoreType.DMA,
            pltpu.SemaphoreType.DMA,
            pltpu.SemaphoreType.DMA((3,)),
            pltpu.SemaphoreType.DMA((3,)),
            pltpu.SemaphoreType.DMA((4,)),
            pltpu.SemaphoreType.DMA((4,)),
            pltpu.SemaphoreType.DMA((len(ORDER),)),
            pltpu.SemaphoreType.DMA((3,)),
            pltpu.SemaphoreType.DMA((3,)),
        ],
        compiler_params=pltpu.CompilerParams(
            collective_id=0, has_side_effects=True, vmem_limit_bytes=40 * 1024 * 1024
        ),
        name="update_sum_gather",
    )(*(pltpu.with_memory_space_constraint(a, pltpu.HBM) for a in args))
    written = pl.pallas_call(
        write_kernel,
        out_shape=[jax.ShapeDtypeStruct(*s) for s in shapes],
        in_specs=[pl.BlockSpec(memory_space=pltpu.VMEM)] * len(shapes),
        out_specs=[pl.BlockSpec(memory_space=pltpu.HBM)] * len(shapes),
        scratch_shapes=[pltpu.SemaphoreType.DMA((len(shapes),))],
        compiler_params=pltpu.CompilerParams(vmem_limit_bytes=1024 * 1024),
        name="write_outputs",
    )(*gathered)
    oq, ok, ov, hq, hk, hv, cq, ck, cv, on = written
    return (
        oq.reshape(D_MODEL, q),
        ok.reshape(D_MODEL, k),
        ov.reshape(D_MODEL, v),
        cq.reshape(q),
        ck.reshape(k),
        cv.reshape(v),
        on.reshape(D_MODEL),
        hq,
        hk,
        hv,
    )


def solution(mesh):
    block = P("shard", "width")
    spread = P(("shard", "width"))
    return jax.shard_map(
        local,
        mesh=mesh,
        in_specs=(block,) * 9 + (spread, spread),
        out_specs=(P(None, "width"),) * 3 + (P("width"),) * 3 + (P(),) + (block,) * 3,
        check_vma=False,
    )
```

```python
import heapq
import itertools

import jax
import jax.numpy as jnp
from jax import lax
from jax.experimental import pallas as pl
from jax.experimental.pallas import tpu as pltpu
from jax.sharding import PartitionSpec as P

D_MODEL = 4096
LEARN_RATE = 0.2
HOLD_RATE = 0.8
MESH = pl.DeviceIdType.MESH

NZ, NX, NC, NW = 8, 4, 2, 4
ROWS = D_MODEL // (NZ * NX * NC)
LANES = 128

PIECES = {
    "A0": (0, 0, 16),
    "A1": (0, 16, 16),
    "A2": (1, 0, 24),
    "B0": (0, 32, 32),
    "B1": (1, 24, 40),
    "B2": (2, 0, 64),
}
KIB = {"A0": 32, "A1": 32, "A2": 12, "B0": 64, "B1": 20, "B2": 32}
STEP = {"+x": (1, 0), "-x": (-1, 0), "+z": (0, 1), "-z": (0, -1)}


def onward(message):
    colour, dx, dz, piece = message
    first = piece in ("A0", "B0")
    out = []

    def along(name, place, farthest, even):
        if place == 0:
            out.extend([("+" + name, 1), ("-" + name, -1)])
        elif 0 < place < farthest - 1 or (place == farthest - 1 and first == even):
            out.append(("+" + name, place + 1))
        elif -farthest + 1 < place < 0:
            out.append(("-" + name, place - 1))
        elif place == -farthest + 1 and first != even:
            out.append(("-" + name, farthest))

    if colour == "A":
        if dz == 0:
            along("x", dx, NX // 2, True)
            out = [(way, (colour, to, 0, piece)) for way, to in out]
            out += [("+z", (colour, dx, 1, piece)), ("-z", (colour, dx, -1, piece))]
        else:
            along("z", dz, NZ // 2, dx % 2 == 0)
            out = [(way, (colour, dx, to, piece)) for way, to in out]
    else:
        if dx == 0:
            along("z", dz, NZ // 2, True)
            out = [(way, (colour, 0, to, piece)) for way, to in out]
            out += [("+x", (colour, 1, dz, piece)), ("-x", (colour, -1, dz, piece))]
        else:
            along("x", dx, NX // 2, dz % 2 == 0)
            out = [(way, (colour, to, dz, piece)) for way, to in out]
    return out


EARLY_X = ("A0", "A1", "A2", "B0", "B1", "B2")
EARLY_Z = (("B0", "B1"), ("A0", "A1"))
EARLY = {"x": EARLY_X, "z": EARLY_Z[0] + EARLY_Z[1]}


def own_hops(pieces, axis):
    hops = [hop for piece in pieces for hop in onward((piece[0], 0, 0, piece))]
    return [(way, message) for way, message in hops if way[1] == axis]


def hops_left(message):
    hops, front = 0, [message]
    while front := [new for old in front for _, new in onward(old)]:
        hops += 1
    return hops


def plan():
    rate, latency, step, slack = 46.65e3 / 1024, 2.2, 0.05, 2.0
    stage_x, stage_z, taken_x, taken_z = 3.7, 4.8, 0.5, 1.05
    free = {way: taken_x if way[1] == "x" else 0.0 for way in STEP}
    waiting = {way: [] for way in STEP}
    events, count = [], itertools.count()

    def issue(now, way, message, width):
        free[way] = max(now, free[way]) + width * KIB[message[3]] / rate
        heapq.heappush(events, (free[way] + latency, message))

    def add(hops):
        for way, message in hops:
            heapq.heappush(waiting[way], (-hops_left(message), next(count), message))

    def sends(now):
        out = []
        for way in STEP:
            while waiting[way] and free[way] - now < slack:
                message = heapq.heappop(waiting[way])[2]
                issue(now, way, message, 1)
                out.append((way, message))
        return out

    for way, message in own_hops(EARLY_X, "x") + own_hops(EARLY_Z[0], "z"):
        issue(0.0, way, message, 2)
    now = max(stage_x, free["+z"])
    for way in ("+z", "-z"):
        free[way] = now + taken_z
    for way, message in own_hops(EARLY_Z[1], "z"):
        issue(now, way, message, 2)
    now += stage_z + 0.2
    events = [(max(at, now), message) for at, message in events]
    heapq.heapify(events)
    for axis in "xz":
        add(own_hops([p for p in PIECES if p not in EARLY[axis]], axis))
    first, steps = sends(now), []
    while events:
        at, message = heapq.heappop(events)
        now = max(now, at) + step
        add(onward(message))
        steps.append((message, sends(now)))
    return first, steps


FIRST, STEPS = plan()
INDEX = {message: i for i, (message, _) in enumerate(STEPS)}
EARLY_WAY = {message: way for axis in "xz" for way, message in own_hops(EARLY[axis], axis)}
SENT = dict.fromkeys(STEP, 0)
for _way, _message in FIRST + [send for _, sends in STEPS for send in sends]:
    SENT[_way] += KIB[_message[3]]


def gather_kernel(
    wq, fq, sq, wk, fk, sk, wv, fv, sv, nt, ns,
    oq, ok, ov, hq, hk, hv, cq, ck, cv, on,
    vq, vk, vv, vn, place, ring_n, ring_m, flat_n, part, line,
    scale, near_q, near_k, near_v, load_sem, part_send, part_recv, line_send, line_recv, norm_send, norm_recv,
    early_send, send_sem, recv_sem, pair_send, pair_recv,
):
    shard = lax.axis_index("shard")
    width = lax.axis_index("width")
    core = lax.rem(shard, NC)
    chip = lax.div(shard, NC)
    x = lax.rem(chip, NX)
    z = lax.div(chip, NX)
    other = 1 - core

    def device(zz, xx, cc):
        return (zz * NX + xx) * NC + cc

    xs = [x] + [lax.rem(x + i, NX) for i in range(1, NX)]
    zs = [z] + [lax.rem(z + i, NZ) for i in range(1, NZ)]

    loads = []
    for i, (src, dst) in enumerate(((nt, vn.at[0]), (ns, vn.at[1]))):
        loads.append(pltpu.make_async_copy(src, dst, load_sem.at[9 + i]))
    for i, src in enumerate((wq, fq, sq, wk, fk, sk, wv, fv, sv)):
        dst = (vq, vk, vv)[i // 3].at[i % 3]
        loads.append(pltpu.make_async_copy(src, dst, load_sem.at[i]))
    for load in loads:
        load.start()

    x_peers = [(device(z, x, other), width)]
    x_peers += [(device(z, xs[i], c), width) for i in range(1, NX) for c in (core, other)]
    z_peers = [(device(zs[i], x, core), width) for i in range(1, NZ)]
    w_peers = [(device(z, x, c), lax.rem(width + i, NW)) for i in range(1, NW) for c in (core, other)]
    barrier = pltpu.get_barrier_semaphore()
    greeted = z_peers + x_peers + w_peers
    for peer in greeted:
        pl.semaphore_signal(barrier, 1, device_id=peer, device_id_type=MESH)

    def send(src, dst, send_to, recv_at, peer):
        copy = pltpu.make_async_remote_copy(
            src_ref=src, dst_ref=dst, send_sem=send_to, recv_sem=recv_at, device_id=peer, device_id_type=MESH
        )
        copy.start()

    def await_bytes(ref, sem):
        pltpu.make_async_copy(ref, ref, sem).wait()

    def await_kib(kib, whole_q, rows_q, rows_k, sem):
        count, kib = divmod(kib, 128)
        if count:
            await_bytes(whole_q(count), sem)
        count, kib = divmod(kib, 16)
        if count:
            await_bytes(rows_q.at[pl.ds(0, 8 * count)], sem)
        count = kib // 4
        if count:
            await_bytes(rows_k.at[pl.ds(0, 8 * count)], sem)

    seat = core * NW + width
    for load in loads[:2]:
        load.wait()
    gain = (vn[0] + vn[1]).astype(jnp.bfloat16).astype(jnp.float32)
    place[...] = jnp.zeros_like(place)
    each = LANES // (NC * NW)
    for i in range(NC * NW):
        place[i : i + 1, i * each : (i + 1) * each] = gain
    ring_n[seat] = place[pl.ds(seat, 1), :]

    group = x * NC + core
    row = 0
    for n, (v, h) in enumerate(((vq, hq), (vk, hk), (vv, hv))):
        for load in loads[2 + 3 * n : 5 + 3 * n]:
            load.wait()
        for j in range(h.shape[1] // LANES):
            at = slice(j * LANES, (j + 1) * LANES)
            hold = HOLD_RATE * v[1, :, at] + v[2, :, at]
            whole = v[0, :, at] - LEARN_RATE * hold
            h[:, at] = whole
            part[group, row : row + 1, :] = jnp.sum(jnp.abs(whole), axis=0, keepdims=True)
            row += 1

    pl.semaphore_wait(barrier, len(greeted))

    ways = list(STEP)
    peers = {
        "+x": (device(z, xs[1], core), width),
        "-x": (device(z, xs[NX - 1], core), width),
        "+z": (device(zs[1], x, core), width),
        "-z": (device(zs[NZ - 1], x, core), width),
    }
    wide = (hq, hk, hv)
    near = (near_q, near_k, near_v)

    def near_ref(way, piece):
        array, start, rows = PIECES[piece]
        return near[array].at[ways.index(way), pl.ds(start, rows)]

    def early(pieces, axis):
        for way, message in own_hops(pieces, axis):
            array, start, rows = PIECES[message[3]]
            src = wide[array].at[pl.ds(start, rows)]
            send(src, near_ref(way, message[3]), early_send.at[ways.index(way)], recv_sem.at[INDEX[message]], peers[way])

    for peer in x_peers:
        send(part.at[group], part.at[group], part_send, part_recv, peer)
    early(EARLY_X, "x")
    early(EARLY_Z[0], "z")
    for peer in [x_peers[0]] + w_peers:
        send(ring_n.at[seat], ring_n.at[seat], norm_send.at[0], norm_recv.at[0], peer)
    await_bytes(part.at[pl.ds(0, 7)], part_recv)
    total = part[0]
    for i in range(1, NX * NC):
        total = total + part[i]
    line[z] = total
    for peer in z_peers:
        send(line.at[z], line.at[z], line_send, line_recv, peer)
    early(EARLY_Z[1], "z")

    await_bytes(line.at[pl.ds(0, 7)], line_recv)
    total = line[0]
    for i in range(1, NZ):
        total = total + line[i]
    column = total * (1.0 / D_MODEL)
    cq[...] = column[0:8]
    ck[...] = column[8:10]
    cv[...] = column[10:12]
    scale[...] = 1.0 / column

    outs = (oq, ok, ov)
    pair = (device(z, x, other), width)

    def block(dx, dz):
        return zs[-dz % NZ] * NX + xs[-dx % NX]

    def piece_ref(dx, dz, piece):
        array, start, rows = PIECES[piece]
        return outs[array].at[block(dx, dz), core, pl.ds(start, rows)]

    def forward(way, message):
        _, dx, dz, piece = message
        ref = piece_ref(dx - STEP[way][0], dz - STEP[way][1], piece)
        send(ref, ref, send_sem.at[ways.index(way)], recv_sem.at[INDEX[message]], peers[way])

    def across(dx, dz, piece):
        ref = piece_ref(dx, dz, piece)
        array = PIECES[piece][0]
        send(ref, ref, pair_send.at[array], pair_recv.at[array], pair)

    def narrow(src, to, piece):
        array, start, rows = PIECES[piece]
        row = sum(h.shape[1] for h in wide[:array]) // LANES
        for j in range(wide[array].shape[1] // LANES):
            at = slice(j * LANES, (j + 1) * LANES)
            part_of = src[:, at] * scale[row + j : row + j + 1, :]
            outs[array][to, core, start : start + rows, at] = part_of.astype(jnp.bfloat16)

    for piece, (array, start, rows) in PIECES.items():
        narrow(wide[array].at[pl.ds(start, rows)], chip, piece)
    for way, message in FIRST:
        forward(way, message)
    for piece in PIECES:
        across(0, 0, piece)
    for step, (message, sends) in enumerate(STEPS):
        _, dx, dz, piece = message
        if message in EARLY_WAY:
            src = near_ref(EARLY_WAY[message], piece)
            await_bytes(src, recv_sem.at[step])
            narrow(src, block(dx, dz), piece)
        else:
            await_bytes(piece_ref(dx, dz, piece), recv_sem.at[step])
        for way, new in sends:
            forward(way, new)
        across(dx, dz, piece)
        if step == len(STEPS) // 4:
            await_bytes(ring_n.at[pl.ds(0, 7)], norm_recv.at[0])
            gain = ring_n[0]
            for i in range(1, NC * NW):
                gain = gain + ring_n[i]
            ring_m[z, x] = gain
            for i in range(1, NX):
                peer = (device(z, xs[i], core), width)
                send(ring_m.at[z, x], ring_m.at[z, x], norm_send.at[1], norm_recv.at[1], peer)
        if step == len(STEPS) // 2:
            await_bytes(ring_m.at[0, pl.ds(0, 3)], norm_recv.at[1])
            for peer in z_peers:
                send(ring_m.at[z], ring_m.at[z], norm_send.at[2], norm_recv.at[2], peer)

    await_bytes(ring_m.at[pl.ds(0, 7)], norm_recv.at[2])
    for i in range(NZ * NX):
        flat_n[i : i + 1, :] = ring_m[i // NX, i % NX]
    on[...] = flat_n[...].astype(jnp.bfloat16)

    for i, out in enumerate(outs):
        await_bytes(out.at[:, other], pair_recv.at[i])
        await_bytes(out.at[:, core], pair_send.at[i])
    for i, way in enumerate(ways):
        await_kib(SENT[way], lambda n: oq.at[pl.ds(0, n), 0], oq.at[0, 0], ok.at[0, 0], send_sem.at[i])
        await_kib(sum(KIB[p] for p in EARLY[way[1]]), lambda n: near_q.at[pl.ds(0, n)], hq, hk, early_send.at[i])
    await_bytes(part.at[pl.ds(0, 7)], part_send)
    await_bytes(line.at[pl.ds(0, 7)], line_send)
    await_bytes(ring_n.at[pl.ds(0, 7)], norm_send.at[0])
    await_bytes(ring_m.at[0, pl.ds(0, 3)], norm_send.at[1])
    await_bytes(ring_m.at[pl.ds(0, 7)], norm_send.at[2])


def write_kernel(*refs):
    count = (len(refs) - 1) // 2
    copies = [pltpu.make_async_copy(refs[i], refs[count + i], refs[-1].at[i]) for i in range(count)]
    for copy in copies:
        copy.start()
    for copy in copies:
        copy.wait()


def local(wq, fq, sq, wk, fk, sk, wv, fv, sv, nt, ns):
    q, k, v = wq.shape[1], wk.shape[1], wv.shape[1]
    cols = (q, k, v)
    tiles = sum(cols) // LANES
    f32, bf16 = jnp.float32, jnp.bfloat16
    shapes = [((NZ * NX, NC, ROWS, n), bf16) for n in cols]
    shapes += [((ROWS, n), f32) for n in cols]
    shapes += [((n // LANES, LANES), f32) for n in cols]
    shapes += [((NZ * NX, LANES), bf16)]
    args = (wq, fq, sq, wk, fk, sk, wv, fv, sv, nt.reshape(1, -1), ns.reshape(1, -1))
    gathered = pl.pallas_call(
        gather_kernel,
        out_shape=[pltpu.VMEM(*s) for s in shapes],
        in_specs=[pl.BlockSpec(memory_space=pltpu.HBM)] * 11,
        out_specs=[pl.BlockSpec(memory_space=pltpu.VMEM)] * len(shapes),
        scratch_shapes=[
            pltpu.VMEM((3, ROWS, q), f32),
            pltpu.VMEM((3, ROWS, k), f32),
            pltpu.VMEM((3, ROWS, v), f32),
            pltpu.VMEM((2, 1, LANES // (NC * NW)), f32),
            pltpu.VMEM((NC * NW, LANES), f32),
            pltpu.VMEM((NC * NW, 1, LANES), f32),
            pltpu.VMEM((NZ, NX, 1, LANES), f32),
            pltpu.VMEM((NZ * NX, LANES), f32),
            pltpu.VMEM((NX * NC, tiles, LANES), f32),
            pltpu.VMEM((NZ, tiles, LANES), f32),
            pltpu.VMEM((tiles, LANES), f32),
            pltpu.VMEM((4, ROWS, q), f32),
            pltpu.VMEM((4, ROWS, k), f32),
            pltpu.VMEM((4, ROWS, v), f32),
            pltpu.SemaphoreType.DMA((11,)),
            pltpu.SemaphoreType.DMA,
            pltpu.SemaphoreType.DMA,
            pltpu.SemaphoreType.DMA,
            pltpu.SemaphoreType.DMA,
            pltpu.SemaphoreType.DMA((3,)),
            pltpu.SemaphoreType.DMA((3,)),
            pltpu.SemaphoreType.DMA((4,)),
            pltpu.SemaphoreType.DMA((4,)),
            pltpu.SemaphoreType.DMA((len(STEPS),)),
            pltpu.SemaphoreType.DMA((3,)),
            pltpu.SemaphoreType.DMA((3,)),
        ],
        compiler_params=pltpu.CompilerParams(
            collective_id=0, has_side_effects=True, vmem_limit_bytes=40 * 1024 * 1024
        ),
        name="update_sum_gather",
    )(*(pltpu.with_memory_space_constraint(a, pltpu.HBM) for a in args))
    written = pl.pallas_call(
        write_kernel,
        out_shape=[jax.ShapeDtypeStruct(*s) for s in shapes],
        in_specs=[pl.BlockSpec(memory_space=pltpu.VMEM)] * len(shapes),
        out_specs=[pl.BlockSpec(memory_space=pltpu.HBM)] * len(shapes),
        scratch_shapes=[pltpu.SemaphoreType.DMA((len(shapes),))],
        compiler_params=pltpu.CompilerParams(vmem_limit_bytes=1024 * 1024),
        name="write_outputs",
    )(*gathered)
    oq, ok, ov, hq, hk, hv, cq, ck, cv, on = written
    return (
        oq.reshape(D_MODEL, q),
        ok.reshape(D_MODEL, k),
        ov.reshape(D_MODEL, v),
        cq.reshape(q),
        ck.reshape(k),
        cv.reshape(v),
        on.reshape(D_MODEL),
        hq,
        hk,
        hv,
    )


def solution(mesh):
    block = P("shard", "width")
    spread = P(("shard", "width"))
    return jax.shard_map(
        local,
        mesh=mesh,
        in_specs=(block,) * 9 + (spread, spread),
        out_specs=(P(None, "width"),) * 3 + (P("width"),) * 3 + (P(),) + (block,) * 3,
        check_vma=False,
    )
```

```python
import heapq
import itertools

import jax
import jax.numpy as jnp
from jax import lax
from jax.experimental import pallas as pl
from jax.experimental.pallas import tpu as pltpu
from jax.sharding import PartitionSpec as P

D_MODEL = 4096
LEARN_RATE = 0.2
HOLD_RATE = 0.8
MESH = pl.DeviceIdType.MESH

NZ, NX, NC, NW = 8, 4, 2, 4
ROWS = D_MODEL // (NZ * NX * NC)
LANES = 128

PIECES = {
    "A0": (0, 0, 16),
    "A1": (0, 16, 16),
    "A2": (1, 0, 24),
    "B0": (0, 32, 32),
    "B1": (1, 24, 40),
    "B2": (2, 0, 64),
}
KIB = {"A0": 32, "A1": 32, "A2": 12, "B0": 64, "B1": 20, "B2": 32}
STEP = {"+x": (1, 0), "-x": (-1, 0), "+z": (0, 1), "-z": (0, -1)}


def onward(message):
    colour, dx, dz, piece = message
    first = piece in ("A0", "B0")
    out = []

    def along(name, place, farthest, even):
        if place == 0:
            out.extend([("+" + name, 1), ("-" + name, -1)])
        elif 0 < place < farthest - 1 or (place == farthest - 1 and first == even):
            out.append(("+" + name, place + 1))
        elif -farthest + 1 < place < 0:
            out.append(("-" + name, place - 1))
        elif place == -farthest + 1 and first != even:
            out.append(("-" + name, farthest))

    if colour == "A":
        if dz == 0:
            along("x", dx, NX // 2, True)
            out = [(way, (colour, to, 0, piece)) for way, to in out]
            out += [("+z", (colour, dx, 1, piece)), ("-z", (colour, dx, -1, piece))]
        else:
            along("z", dz, NZ // 2, dx % 2 == 0)
            out = [(way, (colour, dx, to, piece)) for way, to in out]
    else:
        if dx == 0:
            along("z", dz, NZ // 2, True)
            out = [(way, (colour, 0, to, piece)) for way, to in out]
            out += [("+x", (colour, 1, dz, piece)), ("-x", (colour, -1, dz, piece))]
        else:
            along("x", dx, NX // 2, dz % 2 == 0)
            out = [(way, (colour, to, dz, piece)) for way, to in out]
    return out


EARLY_X = ("A0", "A1", "A2", "B0", "B1", "B2")
EARLY_Z = (("B0", "B1"), ("A0", "A1"))
EARLY = {"x": EARLY_X, "z": EARLY_Z[0] + EARLY_Z[1]}


def own_hops(pieces, axis):
    hops = [hop for piece in pieces for hop in onward((piece[0], 0, 0, piece))]
    return [(way, message) for way, message in hops if way[1] == axis]


def hops_left(message):
    hops, front = 0, [message]
    while front := [new for old in front for _, new in onward(old)]:
        hops += 1
    return hops


def plan():
    rate, latency, step, slack = 46.65e3 / 1024, 2.8, 0.05, 2.0
    stage_x, stage_z, taken_x, taken_z = 4.5, 5.5, 0.5, 1.05
    free = {way: taken_x if way[1] == "x" else 0.0 for way in STEP}
    waiting = {way: [] for way in STEP}
    events, count = [], itertools.count()

    def issue(now, way, message, width):
        free[way] = max(now, free[way]) + width * KIB[message[3]] / rate
        heapq.heappush(events, (free[way] + latency, message))

    def add(hops):
        for way, message in hops:
            heapq.heappush(waiting[way], (-hops_left(message), next(count), message))

    def sends(now):
        out = []
        for way in STEP:
            while waiting[way] and free[way] - now < slack:
                message = heapq.heappop(waiting[way])[2]
                issue(now, way, message, 1)
                out.append((way, message))
        return out

    for way, message in own_hops(EARLY_X, "x") + own_hops(EARLY_Z[0], "z"):
        issue(0.0, way, message, 2)
    now = max(stage_x, free["+z"])
    for way in ("+z", "-z"):
        free[way] = now + taken_z
    for way, message in own_hops(EARLY_Z[1], "z"):
        issue(now, way, message, 2)
    now += stage_z + 0.2
    events = [(max(at, now), message) for at, message in events]
    heapq.heapify(events)
    for axis in "xz":
        add(own_hops([p for p in PIECES if p not in EARLY[axis]], axis))
    first, steps = sends(now), []
    while events:
        at, message = heapq.heappop(events)
        now = max(now, at) + step
        add(onward(message))
        steps.append((message, sends(now)))
    return first, steps


FIRST, STEPS = plan()
INDEX = {message: i for i, (message, _) in enumerate(STEPS)}
EARLY_WAY = {message: way for axis in "xz" for way, message in own_hops(EARLY[axis], axis)}
SENT = dict.fromkeys(STEP, 0)
for _way, _message in FIRST + [send for _, sends in STEPS for send in sends]:
    SENT[_way] += KIB[_message[3]]


def gather_kernel(
    wq, fq, sq, wk, fk, sk, wv, fv, sv, nt, ns,
    oq, ok, ov, hq, hk, hv, cq, ck, cv, on,
    vq, vk, vv, vn, place, ring_n, ring_m, flat_n, part, line,
    scale, near_q, near_k, near_v, load_sem, part_send, part_recv, line_send, line_recv, norm_send, norm_recv,
    early_send, send_sem, recv_sem, pair_send, pair_recv,
):
    shard = lax.axis_index("shard")
    width = lax.axis_index("width")
    core = lax.rem(shard, NC)
    chip = lax.div(shard, NC)
    x = lax.rem(chip, NX)
    z = lax.div(chip, NX)
    other = 1 - core

    def device(zz, xx, cc):
        return (zz * NX + xx) * NC + cc

    xs = [x] + [lax.rem(x + i, NX) for i in range(1, NX)]
    zs = [z] + [lax.rem(z + i, NZ) for i in range(1, NZ)]

    loads = []
    for i, (src, dst) in enumerate(((nt, vn.at[0]), (ns, vn.at[1]))):
        loads.append(pltpu.make_async_copy(src, dst, load_sem.at[9 + i]))
    for i, src in enumerate((wq, fq, sq, wk, fk, sk, wv, fv, sv)):
        dst = (vq, vk, vv)[i // 3].at[i % 3]
        loads.append(pltpu.make_async_copy(src, dst, load_sem.at[i]))
    for load in loads:
        load.start()

    x_peers = [(device(z, xs[i], c), width) for i in (2, 1, 3) for c in (other, core)]
    x_peers += [(device(z, x, other), width)]
    z_peers = [(device(zs[i], x, core), width) for i in (4, 3, 5, 2, 6, 1, 7)]
    w_peers = [(device(z, x, c), lax.rem(width + i, NW)) for i in range(1, NW) for c in (core, other)]
    barrier = pltpu.get_barrier_semaphore()
    greeted = z_peers + x_peers + w_peers
    for peer in greeted:
        pl.semaphore_signal(barrier, 1, device_id=peer, device_id_type=MESH)

    def send(src, dst, send_to, recv_at, peer):
        copy = pltpu.make_async_remote_copy(
            src_ref=src, dst_ref=dst, send_sem=send_to, recv_sem=recv_at, device_id=peer, device_id_type=MESH
        )
        copy.start()

    def await_bytes(ref, sem):
        pltpu.make_async_copy(ref, ref, sem).wait()

    def await_kib(kib, whole_q, rows_q, rows_k, sem):
        count, kib = divmod(kib, 128)
        if count:
            await_bytes(whole_q(count), sem)
        count, kib = divmod(kib, 16)
        if count:
            await_bytes(rows_q.at[pl.ds(0, 8 * count)], sem)
        count = kib // 4
        if count:
            await_bytes(rows_k.at[pl.ds(0, 8 * count)], sem)

    seat = core * NW + width
    for load in loads[:2]:
        load.wait()
    gain = (vn[0] + vn[1]).astype(jnp.bfloat16).astype(jnp.float32)
    place[...] = jnp.zeros_like(place)
    each = LANES // (NC * NW)
    for i in range(NC * NW):
        place[i : i + 1, i * each : (i + 1) * each] = gain
    ring_n[seat] = place[pl.ds(seat, 1), :]

    group = x * NC + core
    row = 0
    for n, (v, h) in enumerate(((vq, hq), (vk, hk), (vv, hv))):
        for load in loads[2 + 3 * n : 5 + 3 * n]:
            load.wait()
        for j in range(h.shape[1] // LANES):
            at = slice(j * LANES, (j + 1) * LANES)
            hold = HOLD_RATE * v[1, :, at] + v[2, :, at]
            whole = v[0, :, at] - LEARN_RATE * hold
            h[:, at] = whole
            part[group, row : row + 1, :] = jnp.sum(jnp.abs(whole), axis=0, keepdims=True)
            row += 1

    pl.semaphore_wait(barrier, len(greeted))

    ways = list(STEP)
    peers = {
        "+x": (device(z, xs[1], core), width),
        "-x": (device(z, xs[NX - 1], core), width),
        "+z": (device(zs[1], x, core), width),
        "-z": (device(zs[NZ - 1], x, core), width),
    }
    wide = (hq, hk, hv)
    near = (near_q, near_k, near_v)

    def near_ref(way, piece):
        array, start, rows = PIECES[piece]
        return near[array].at[ways.index(way), pl.ds(start, rows)]

    def early(pieces, axis):
        for way, message in own_hops(pieces, axis):
            array, start, rows = PIECES[message[3]]
            src = wide[array].at[pl.ds(start, rows)]
            send(src, near_ref(way, message[3]), early_send.at[ways.index(way)], recv_sem.at[INDEX[message]], peers[way])

    for peer in x_peers:
        send(part.at[group], part.at[group], part_send, part_recv, peer)
    early(EARLY_X, "x")
    early(EARLY_Z[0], "z")
    for peer in [x_peers[-1]] + w_peers:
        send(ring_n.at[seat], ring_n.at[seat], norm_send.at[0], norm_recv.at[0], peer)
    await_bytes(part.at[pl.ds(0, 7)], part_recv)
    total = part[0]
    for i in range(1, NX * NC):
        total = total + part[i]
    line[z] = total
    for peer in z_peers:
        send(line.at[z], line.at[z], line_send, line_recv, peer)
    early(EARLY_Z[1], "z")

    await_bytes(line.at[pl.ds(0, 7)], line_recv)
    total = line[0]
    for i in range(1, NZ):
        total = total + line[i]
    column = total * (1.0 / D_MODEL)
    cq[...] = column[0:8]
    ck[...] = column[8:10]
    cv[...] = column[10:12]
    scale[...] = 1.0 / column

    outs = (oq, ok, ov)
    pair = (device(z, x, other), width)

    def block(dx, dz):
        return zs[-dz % NZ] * NX + xs[-dx % NX]

    def piece_ref(dx, dz, piece):
        array, start, rows = PIECES[piece]
        return outs[array].at[block(dx, dz), core, pl.ds(start, rows)]

    def forward(way, message):
        _, dx, dz, piece = message
        ref = piece_ref(dx - STEP[way][0], dz - STEP[way][1], piece)
        send(ref, ref, send_sem.at[ways.index(way)], recv_sem.at[INDEX[message]], peers[way])

    def across(dx, dz, piece):
        ref = piece_ref(dx, dz, piece)
        array = PIECES[piece][0]
        send(ref, ref, pair_send.at[array], pair_recv.at[array], pair)

    def narrow(src, to, piece):
        array, start, rows = PIECES[piece]
        row = sum(h.shape[1] for h in wide[:array]) // LANES
        for j in range(wide[array].shape[1] // LANES):
            at = slice(j * LANES, (j + 1) * LANES)
            part_of = src[:, at] * scale[row + j : row + j + 1, :]
            outs[array][to, core, start : start + rows, at] = part_of.astype(jnp.bfloat16)

    for piece, (array, start, rows) in PIECES.items():
        narrow(wide[array].at[pl.ds(start, rows)], chip, piece)
    for way, message in FIRST:
        forward(way, message)
    for piece in PIECES:
        across(0, 0, piece)
    for step, (message, sends) in enumerate(STEPS):
        _, dx, dz, piece = message
        if message in EARLY_WAY:
            src = near_ref(EARLY_WAY[message], piece)
            await_bytes(src, recv_sem.at[step])
            narrow(src, block(dx, dz), piece)
        else:
            await_bytes(piece_ref(dx, dz, piece), recv_sem.at[step])
        for way, new in sends:
            forward(way, new)
        across(dx, dz, piece)
        if step == len(STEPS) // 4:
            await_bytes(ring_n.at[pl.ds(0, 7)], norm_recv.at[0])
            gain = ring_n[0]
            for i in range(1, NC * NW):
                gain = gain + ring_n[i]
            ring_m[z, x] = gain
            for i in range(1, NX):
                peer = (device(z, xs[i], core), width)
                send(ring_m.at[z, x], ring_m.at[z, x], norm_send.at[1], norm_recv.at[1], peer)
        if step == len(STEPS) // 2:
            await_bytes(ring_m.at[0, pl.ds(0, 3)], norm_recv.at[1])
            for peer in z_peers:
                send(ring_m.at[z], ring_m.at[z], norm_send.at[2], norm_recv.at[2], peer)

    await_bytes(ring_m.at[pl.ds(0, 7)], norm_recv.at[2])
    for i in range(NZ * NX):
        flat_n[i : i + 1, :] = ring_m[i // NX, i % NX]
    on[...] = flat_n[...].astype(jnp.bfloat16)

    for i, out in enumerate(outs):
        await_bytes(out.at[:, other], pair_recv.at[i])
        await_bytes(out.at[:, core], pair_send.at[i])
    for i, way in enumerate(ways):
        await_kib(SENT[way], lambda n: oq.at[pl.ds(0, n), 0], oq.at[0, 0], ok.at[0, 0], send_sem.at[i])
        await_kib(sum(KIB[p] for p in EARLY[way[1]]), lambda n: near_q.at[pl.ds(0, n)], hq, hk, early_send.at[i])
    await_bytes(part.at[pl.ds(0, 7)], part_send)
    await_bytes(line.at[pl.ds(0, 7)], line_send)
    await_bytes(ring_n.at[pl.ds(0, 7)], norm_send.at[0])
    await_bytes(ring_m.at[0, pl.ds(0, 3)], norm_send.at[1])
    await_bytes(ring_m.at[pl.ds(0, 7)], norm_send.at[2])


def write_kernel(*refs):
    count = (len(refs) - 1) // 2
    copies = [pltpu.make_async_copy(refs[i], refs[count + i], refs[-1].at[i]) for i in range(count)]
    for copy in copies:
        copy.start()
    for copy in copies:
        copy.wait()


def local(wq, fq, sq, wk, fk, sk, wv, fv, sv, nt, ns):
    q, k, v = wq.shape[1], wk.shape[1], wv.shape[1]
    cols = (q, k, v)
    tiles = sum(cols) // LANES
    f32, bf16 = jnp.float32, jnp.bfloat16
    shapes = [((NZ * NX, NC, ROWS, n), bf16) for n in cols]
    shapes += [((ROWS, n), f32) for n in cols]
    shapes += [((n // LANES, LANES), f32) for n in cols]
    shapes += [((NZ * NX, LANES), bf16)]
    args = (wq, fq, sq, wk, fk, sk, wv, fv, sv, nt.reshape(1, -1), ns.reshape(1, -1))
    gathered = pl.pallas_call(
        gather_kernel,
        out_shape=[pltpu.VMEM(*s) for s in shapes],
        in_specs=[pl.BlockSpec(memory_space=pltpu.HBM)] * 11,
        out_specs=[pl.BlockSpec(memory_space=pltpu.VMEM)] * len(shapes),
        scratch_shapes=[
            pltpu.VMEM((3, ROWS, q), f32),
            pltpu.VMEM((3, ROWS, k), f32),
            pltpu.VMEM((3, ROWS, v), f32),
            pltpu.VMEM((2, 1, LANES // (NC * NW)), f32),
            pltpu.VMEM((NC * NW, LANES), f32),
            pltpu.VMEM((NC * NW, 1, LANES), f32),
            pltpu.VMEM((NZ, NX, 1, LANES), f32),
            pltpu.VMEM((NZ * NX, LANES), f32),
            pltpu.VMEM((NX * NC, tiles, LANES), f32),
            pltpu.VMEM((NZ, tiles, LANES), f32),
            pltpu.VMEM((tiles, LANES), f32),
            pltpu.VMEM((4, ROWS, q), f32),
            pltpu.VMEM((4, ROWS, k), f32),
            pltpu.VMEM((4, ROWS, v), f32),
            pltpu.SemaphoreType.DMA((11,)),
            pltpu.SemaphoreType.DMA,
            pltpu.SemaphoreType.DMA,
            pltpu.SemaphoreType.DMA,
            pltpu.SemaphoreType.DMA,
            pltpu.SemaphoreType.DMA((3,)),
            pltpu.SemaphoreType.DMA((3,)),
            pltpu.SemaphoreType.DMA((4,)),
            pltpu.SemaphoreType.DMA((4,)),
            pltpu.SemaphoreType.DMA((len(STEPS),)),
            pltpu.SemaphoreType.DMA((3,)),
            pltpu.SemaphoreType.DMA((3,)),
        ],
        compiler_params=pltpu.CompilerParams(
            collective_id=0, has_side_effects=True, vmem_limit_bytes=40 * 1024 * 1024
        ),
        name="update_sum_gather",
    )(*(pltpu.with_memory_space_constraint(a, pltpu.HBM) for a in args))
    written = pl.pallas_call(
        write_kernel,
        out_shape=[jax.ShapeDtypeStruct(*s) for s in shapes],
        in_specs=[pl.BlockSpec(memory_space=pltpu.VMEM)] * len(shapes),
        out_specs=[pl.BlockSpec(memory_space=pltpu.HBM)] * len(shapes),
        scratch_shapes=[pltpu.SemaphoreType.DMA((len(shapes),))],
        compiler_params=pltpu.CompilerParams(vmem_limit_bytes=1024 * 1024),
        name="write_outputs",
    )(*gathered)
    oq, ok, ov, hq, hk, hv, cq, ck, cv, on = written
    return (
        oq.reshape(D_MODEL, q),
        ok.reshape(D_MODEL, k),
        ov.reshape(D_MODEL, v),
        cq.reshape(q),
        ck.reshape(k),
        cv.reshape(v),
        on.reshape(D_MODEL),
        hq,
        hk,
        hv,
    )


def solution(mesh):
    block = P("shard", "width")
    spread = P(("shard", "width"))
    return jax.shard_map(
        local,
        mesh=mesh,
        in_specs=(block,) * 9 + (spread, spread),
        out_specs=(P(None, "width"),) * 3 + (P("width"),) * 3 + (P(),) + (block,) * 3,
        check_vma=False,
    )
```

```python
import heapq
import itertools

import jax
import jax.numpy as jnp
from jax import lax
from jax.experimental import pallas as pl
from jax.experimental.pallas import tpu as pltpu
from jax.sharding import PartitionSpec as P

D_MODEL = 4096
LEARN_RATE = 0.2
HOLD_RATE = 0.8
MESH = pl.DeviceIdType.MESH

NZ, NX, NC, NW = 8, 4, 2, 4
ROWS = D_MODEL // (NZ * NX * NC)
LANES = 128

PIECES = {
    "A0": (0, 0, 16),
    "A1": (0, 16, 16),
    "A2": (1, 0, 24),
    "B0": (0, 32, 32),
    "B1": (1, 24, 40),
    "B2": (2, 0, 64),
}
KIB = {"A0": 32, "A1": 32, "A2": 12, "B0": 64, "B1": 20, "B2": 32}
STEP = {"+x": (1, 0), "-x": (-1, 0), "+z": (0, 1), "-z": (0, -1)}


def onward(message):
    colour, dx, dz, piece = message
    first = piece in ("A0", "B0")
    out = []

    def along(name, place, farthest, even):
        if place == 0:
            out.extend([("+" + name, 1), ("-" + name, -1)])
        elif 0 < place < farthest - 1 or (place == farthest - 1 and first == even):
            out.append(("+" + name, place + 1))
        elif -farthest + 1 < place < 0:
            out.append(("-" + name, place - 1))
        elif place == -farthest + 1 and first != even:
            out.append(("-" + name, farthest))

    if colour == "A":
        if dz == 0:
            along("x", dx, NX // 2, True)
            out = [(way, (colour, to, 0, piece)) for way, to in out]
            out += [("+z", (colour, dx, 1, piece)), ("-z", (colour, dx, -1, piece))]
        else:
            along("z", dz, NZ // 2, dx % 2 == 0)
            out = [(way, (colour, dx, to, piece)) for way, to in out]
    else:
        if dx == 0:
            along("z", dz, NZ // 2, True)
            out = [(way, (colour, 0, to, piece)) for way, to in out]
            out += [("+x", (colour, 1, dz, piece)), ("-x", (colour, -1, dz, piece))]
        else:
            along("x", dx, NX // 2, dz % 2 == 0)
            out = [(way, (colour, to, dz, piece)) for way, to in out]
    return out


EARLY_X = ("A0", "A1", "A2", "B0", "B1", "B2")
EARLY_Z = (("B0", "B1"), ("A0", "A1"))
EARLY = {"x": EARLY_X, "z": EARLY_Z[0] + EARLY_Z[1]}


def own_hops(pieces, axis):
    hops = [hop for piece in pieces for hop in onward((piece[0], 0, 0, piece))]
    return [(way, message) for way, message in hops if way[1] == axis]


def hops_left(message):
    hops, front = 0, [message]
    while front := [new for old in front for _, new in onward(old)]:
        hops += 1
    return hops


def plan():
    rate, latency, step, slack = 46.65e3 / 1024, 2.8, 0.05, 2.0
    stage_x, stage_z, taken_x, taken_z = 4.5, 5.5, 0.5, 1.05
    free = {way: taken_x if way[1] == "x" else 0.0 for way in STEP}
    waiting = {way: [] for way in STEP}
    events, count = [], itertools.count()

    def issue(now, way, message, width):
        free[way] = max(now, free[way]) + width * KIB[message[3]] / rate
        heapq.heappush(events, (free[way] + latency, message))

    def add(hops):
        for way, message in hops:
            heapq.heappush(waiting[way], (-hops_left(message), next(count), message))

    def sends(now):
        out = []
        for way in STEP:
            while waiting[way] and free[way] - now < slack:
                message = heapq.heappop(waiting[way])[2]
                issue(now, way, message, 1)
                out.append((way, message))
        return out

    for way, message in own_hops(EARLY_X, "x") + own_hops(EARLY_Z[0], "z"):
        issue(0.0, way, message, 2)
    now = max(stage_x, free["+z"])
    for way in ("+z", "-z"):
        free[way] = now + taken_z
    for way, message in own_hops(EARLY_Z[1], "z"):
        issue(now, way, message, 2)
    now += stage_z + 0.2
    events = [(max(at, now), message) for at, message in events]
    heapq.heapify(events)
    for axis in "xz":
        add(own_hops([p for p in PIECES if p not in EARLY[axis]], axis))
    first, steps = sends(now), []
    while events:
        at, message = heapq.heappop(events)
        now = max(now, at) + step
        add(onward(message))
        steps.append((message, sends(now)))
    return first, steps


FIRST, STEPS = plan()
INDEX = {message: i for i, (message, _) in enumerate(STEPS)}
EARLY_WAY = {message: way for axis in "xz" for way, message in own_hops(EARLY[axis], axis)}
SENT = sum(KIB[message[3]] for _, message in FIRST + [hop for _, sends in STEPS for hop in sends])


def slots():
    turn = {"+x": "-x", "-x": "+x", "+z": "-z", "-z": "+z"}
    sent = [(-1, way, message) for axis in "xz" for way, message in own_hops(EARLY[axis], axis)]
    sent += [(-1, way, message) for way, message in FIRST]
    sent += [(step, way, message) for step, (_, sends) in enumerate(STEPS) for way, message in sends]

    def known(old, way):
        later = [INDEX[m] for at, back, m in sent if back == turn[way] and at >= max(0, INDEX[old])]
        return min(later, default=len(STEPS))

    last, slot = [], {}
    for at, way, message in sorted(sent, key=lambda entry: (entry[0], INDEX[entry[2]])):
        free = [i for i, old in enumerate(last) if at >= 0 and known(old, way) <= at]
        if free:
            slot[message] = free[0]
            last[free[0]] = message
        else:
            slot[message] = len(last)
            last.append(message)
    return slot


SLOT = slots()


def gather_kernel(
    wq, fq, sq, wk, fk, sk, wv, fv, sv, nt, ns,
    oq, ok, ov, hq, hk, hv, cq, ck, cv, on,
    vq, vk, vv, vn, place, ring_n, ring_m, flat_n, part, line,
    scale, near_q, near_k, near_v, load_sem, part_recv, line_recv, norm_send, norm_recv,
    early_send, send_sem, recv_sem, pair_send, pair_recv,
):
    shard = lax.axis_index("shard")
    width = lax.axis_index("width")
    core = lax.rem(shard, NC)
    chip = lax.div(shard, NC)
    x = lax.rem(chip, NX)
    z = lax.div(chip, NX)
    other = 1 - core

    def device(zz, xx, cc):
        return (zz * NX + xx) * NC + cc

    xs = [x] + [lax.rem(x + i, NX) for i in range(1, NX)]
    zs = [z] + [lax.rem(z + i, NZ) for i in range(1, NZ)]

    loads = []
    for i, (src, dst) in enumerate(((nt, vn.at[0]), (ns, vn.at[1]))):
        loads.append(pltpu.make_async_copy(src, dst, load_sem.at[3 + i]))
    for i, src in enumerate((wq, fq, sq, wk, fk, sk, wv, fv, sv)):
        dst = (vq, vk, vv)[i // 3].at[i % 3]
        loads.append(pltpu.make_async_copy(src, dst, load_sem.at[i // 3]))
    for load in loads:
        load.start()

    x_peers = [(device(z, xs[i], c), width) for i in (2, 1, 3) for c in (other, core)]
    x_peers += [(device(z, x, other), width)]
    z_peers = [(device(zs[i], x, core), width) for i in (4, 3, 5, 2, 6, 1, 7)]
    w_peers = [(device(z, x, c), lax.rem(width + i, NW)) for i in range(1, NW) for c in (core, other)]
    barrier = pltpu.get_barrier_semaphore()
    greeted = z_peers + x_peers + w_peers
    for peer in greeted:
        pl.semaphore_signal(barrier, 1, device_id=peer, device_id_type=MESH)

    def send(src, dst, send_to, recv_at, peer):
        copy = pltpu.make_async_remote_copy(
            src_ref=src, dst_ref=dst, send_sem=send_to, recv_sem=recv_at, device_id=peer, device_id_type=MESH
        )
        copy.start()

    def await_bytes(ref, sem):
        pltpu.make_async_copy(ref, ref, sem).wait()

    def await_kib(kib, whole_q, rows_q, rows_k, sem):
        count, kib = divmod(kib, 128)
        if count:
            await_bytes(whole_q(count), sem)
        count, kib = divmod(kib, 16)
        if count:
            await_bytes(rows_q.at[pl.ds(0, 8 * count)], sem)
        count = kib // 4
        if count:
            await_bytes(rows_k.at[pl.ds(0, 8 * count)], sem)

    seat = core * NW + width
    for load in loads[:2]:
        load.wait()
    gain = (vn[0] + vn[1]).astype(jnp.bfloat16).astype(jnp.float32)
    place[...] = jnp.zeros_like(place)
    each = LANES // (NC * NW)
    for i in range(NC * NW):
        place[i : i + 1, i * each : (i + 1) * each] = gain
    ring_n[seat] = place[pl.ds(seat, 1), :]

    group = x * NC + core
    row = 0
    for n, (v, h) in enumerate(((vq, hq), (vk, hk), (vv, hv))):
        await_bytes(v, load_sem.at[n])
        for j in range(h.shape[1] // LANES):
            at = slice(j * LANES, (j + 1) * LANES)
            hold = HOLD_RATE * v[1, :, at] + v[2, :, at]
            whole = v[0, :, at] - LEARN_RATE * hold
            h[:, at] = whole
            part[group, row : row + 1, :] = jnp.sum(jnp.abs(whole), axis=0, keepdims=True)
            row += 1

    pl.semaphore_wait(barrier, len(greeted))

    ways = list(STEP)
    peers = {
        "+x": (device(z, xs[1], core), width),
        "-x": (device(z, xs[NX - 1], core), width),
        "+z": (device(zs[1], x, core), width),
        "-z": (device(zs[NZ - 1], x, core), width),
    }
    wide = (hq, hk, hv)
    near = (near_q, near_k, near_v)

    def near_ref(way, piece):
        array, start, rows = PIECES[piece]
        return near[array].at[ways.index(way), pl.ds(start, rows)]

    def early(pieces, axis):
        for way, message in own_hops(pieces, axis):
            array, start, rows = PIECES[message[3]]
            src = wide[array].at[pl.ds(start, rows)]
            send(src, near_ref(way, message[3]), early_send, recv_sem.at[SLOT[message]], peers[way])

    for peer in x_peers:
        send(part.at[group], part.at[group], norm_send, part_recv, peer)
    early(EARLY_X, "x")
    early(EARLY_Z[0], "z")
    for peer in [x_peers[-1]] + w_peers:
        send(ring_n.at[seat], ring_n.at[seat], norm_send, norm_recv.at[0], peer)
    await_bytes(part.at[pl.ds(0, 7)], part_recv)
    total = part[0]
    for i in range(1, NX * NC):
        total = total + part[i]
    line[z] = total
    for peer in z_peers:
        send(line.at[z], line.at[z], norm_send, line_recv, peer)
    early(EARLY_Z[1], "z")

    await_bytes(line.at[pl.ds(0, 7)], line_recv)
    total = line[0]
    for i in range(1, NZ):
        total = total + line[i]
    column = total * (1.0 / D_MODEL)
    cq[...] = column[0:8]
    ck[...] = column[8:10]
    cv[...] = column[10:12]
    scale[...] = 1.0 / column

    outs = (oq, ok, ov)
    pair = (device(z, x, other), width)

    def block(dx, dz):
        return zs[-dz % NZ] * NX + xs[-dx % NX]

    def piece_ref(dx, dz, piece):
        array, start, rows = PIECES[piece]
        return outs[array].at[block(dx, dz), core, pl.ds(start, rows)]

    def forward(way, message):
        _, dx, dz, piece = message
        ref = piece_ref(dx - STEP[way][0], dz - STEP[way][1], piece)
        send(ref, ref, send_sem, recv_sem.at[SLOT[message]], peers[way])

    def across(dx, dz, piece):
        ref = piece_ref(dx, dz, piece)
        array = PIECES[piece][0]
        send(ref, ref, pair_send.at[array], pair_recv.at[array], pair)

    def narrow(src, to, piece):
        array, start, rows = PIECES[piece]
        row = sum(h.shape[1] for h in wide[:array]) // LANES
        for j in range(wide[array].shape[1] // LANES):
            at = slice(j * LANES, (j + 1) * LANES)
            part_of = src[:, at] * scale[row + j : row + j + 1, :]
            outs[array][to, core, start : start + rows, at] = part_of.astype(jnp.bfloat16)

    for piece, (array, start, rows) in PIECES.items():
        narrow(wide[array].at[pl.ds(start, rows)], chip, piece)
    for way, message in FIRST:
        forward(way, message)
    for piece in PIECES:
        across(0, 0, piece)
    for step, (message, sends) in enumerate(STEPS):
        _, dx, dz, piece = message
        if message in EARLY_WAY:
            src = near_ref(EARLY_WAY[message], piece)
            await_bytes(src, recv_sem.at[SLOT[message]])
            narrow(src, block(dx, dz), piece)
        else:
            await_bytes(piece_ref(dx, dz, piece), recv_sem.at[SLOT[message]])
        for way, new in sends:
            forward(way, new)
        across(dx, dz, piece)
        if step == len(STEPS) // 4:
            await_bytes(ring_n.at[pl.ds(0, 7)], norm_recv.at[0])
            gain = ring_n[0]
            for i in range(1, NC * NW):
                gain = gain + ring_n[i]
            ring_m[z, x] = gain
            for i in range(1, NX):
                peer = (device(z, xs[i], core), width)
                send(ring_m.at[z, x], ring_m.at[z, x], norm_send, norm_recv.at[1], peer)
        if step == len(STEPS) // 2:
            await_bytes(ring_m.at[0, pl.ds(0, 3)], norm_recv.at[1])
            for peer in z_peers:
                send(ring_m.at[z], ring_m.at[z], norm_send, norm_recv.at[2], peer)

    await_bytes(ring_m.at[pl.ds(0, 7)], norm_recv.at[2])
    for i in range(NZ * NX):
        flat_n[i : i + 1, :] = ring_m[i // NX, i % NX]
    on[...] = flat_n[...].astype(jnp.bfloat16)

    for i, out in enumerate(outs):
        await_bytes(out.at[:, other], pair_recv.at[i])
        await_bytes(out.at[:, core], pair_send.at[i])
    half = SENT // 8 * 4
    for kib in (half, SENT - half):
        await_kib(kib, lambda n: oq.at[pl.ds(0, n), 0], oq.at[0, 0], ok.at[0, 0], send_sem)
    early_kib = 2 * sum(KIB[p] for axis in "xz" for p in EARLY[axis])
    for _ in range(2):
        await_kib(early_kib // 2, lambda n: near_q.at[pl.ds(0, n)], hq, hk, early_send)
    await_bytes(part.at[pl.ds(0, 7)], norm_send)
    await_bytes(line.at[pl.ds(0, 7)], norm_send)
    await_bytes(ring_n.at[pl.ds(0, 7)], norm_send)
    await_bytes(ring_m.at[0, pl.ds(0, 3)], norm_send)
    await_bytes(ring_m.at[pl.ds(0, 7)], norm_send)


def write_kernel(*refs):
    count = (len(refs) - 1) // 2
    copies = [pltpu.make_async_copy(refs[i], refs[count + i], refs[-1].at[i]) for i in range(count)]
    for copy in copies:
        copy.start()
    for copy in copies:
        copy.wait()


def local(wq, fq, sq, wk, fk, sk, wv, fv, sv, nt, ns):
    q, k, v = wq.shape[1], wk.shape[1], wv.shape[1]
    cols = (q, k, v)
    tiles = sum(cols) // LANES
    f32, bf16 = jnp.float32, jnp.bfloat16
    shapes = [((NZ * NX, NC, ROWS, n), bf16) for n in cols]
    shapes += [((ROWS, n), f32) for n in cols]
    shapes += [((n // LANES, LANES), f32) for n in cols]
    shapes += [((NZ * NX, LANES), bf16)]
    args = (wq, fq, sq, wk, fk, sk, wv, fv, sv, nt.reshape(1, -1), ns.reshape(1, -1))
    gathered = pl.pallas_call(
        gather_kernel,
        out_shape=[pltpu.VMEM(*s) for s in shapes],
        in_specs=[pl.BlockSpec(memory_space=pltpu.HBM)] * 11,
        out_specs=[pl.BlockSpec(memory_space=pltpu.VMEM)] * len(shapes),
        scratch_shapes=[
            pltpu.VMEM((3, ROWS, q), f32),
            pltpu.VMEM((3, ROWS, k), f32),
            pltpu.VMEM((3, ROWS, v), f32),
            pltpu.VMEM((2, 1, LANES // (NC * NW)), f32),
            pltpu.VMEM((NC * NW, LANES), f32),
            pltpu.VMEM((NC * NW, 1, LANES), f32),
            pltpu.VMEM((NZ, NX, 1, LANES), f32),
            pltpu.VMEM((NZ * NX, LANES), f32),
            pltpu.VMEM((NX * NC, tiles, LANES), f32),
            pltpu.VMEM((NZ, tiles, LANES), f32),
            pltpu.VMEM((tiles, LANES), f32),
            pltpu.VMEM((4, ROWS, q), f32),
            pltpu.VMEM((4, ROWS, k), f32),
            pltpu.VMEM((4, ROWS, v), f32),
            pltpu.SemaphoreType.DMA((5,)),
            pltpu.SemaphoreType.DMA,
            pltpu.SemaphoreType.DMA,
            pltpu.SemaphoreType.DMA,
            pltpu.SemaphoreType.DMA((3,)),
            pltpu.SemaphoreType.DMA,
            pltpu.SemaphoreType.DMA,
            pltpu.SemaphoreType.DMA((1 + max(SLOT.values()),)),
            pltpu.SemaphoreType.DMA((3,)),
            pltpu.SemaphoreType.DMA((3,)),
        ],
        compiler_params=pltpu.CompilerParams(
            collective_id=0, has_side_effects=True, vmem_limit_bytes=40 * 1024 * 1024
        ),
        name="update_sum_gather",
    )(*(pltpu.with_memory_space_constraint(a, pltpu.HBM) for a in args))
    written = pl.pallas_call(
        write_kernel,
        out_shape=[jax.ShapeDtypeStruct(*s) for s in shapes],
        in_specs=[pl.BlockSpec(memory_space=pltpu.VMEM)] * len(shapes),
        out_specs=[pl.BlockSpec(memory_space=pltpu.HBM)] * len(shapes),
        scratch_shapes=[pltpu.SemaphoreType.DMA((len(shapes),))],
        compiler_params=pltpu.CompilerParams(vmem_limit_bytes=1024 * 1024),
        name="write_outputs",
    )(*gathered)
    oq, ok, ov, hq, hk, hv, cq, ck, cv, on = written
    return (
        oq.reshape(D_MODEL, q),
        ok.reshape(D_MODEL, k),
        ov.reshape(D_MODEL, v),
        cq.reshape(q),
        ck.reshape(k),
        cv.reshape(v),
        on.reshape(D_MODEL),
        hq,
        hk,
        hv,
    )


def solution(mesh):
    block = P("shard", "width")
    spread = P(("shard", "width"))
    return jax.shard_map(
        local,
        mesh=mesh,
        in_specs=(block,) * 9 + (spread, spread),
        out_specs=(P(None, "width"),) * 3 + (P("width"),) * 3 + (P(),) + (block,) * 3,
        check_vma=False,
    )
```

```python
import heapq
import itertools

import jax
import jax.numpy as jnp
from jax import lax
from jax.experimental import pallas as pl
from jax.experimental.pallas import tpu as pltpu
from jax.sharding import PartitionSpec as P

D_MODEL = 4096
LEARN_RATE = 0.2
HOLD_RATE = 0.8
MESH = pl.DeviceIdType.MESH

NZ, NX, NC, NW = 8, 4, 2, 4
ROWS = D_MODEL // (NZ * NX * NC)
LANES = 128

PIECES = {
    "A0": (0, 0, 16),
    "A1": (0, 16, 16),
    "A2": (1, 0, 24),
    "B0": (0, 32, 16),
    "B3": (0, 48, 16),
    "B1": (1, 24, 40),
    "B2": (2, 0, 64),
}
KIB = {"A0": 32, "A1": 32, "A2": 12, "B0": 32, "B3": 32, "B1": 20, "B2": 32}
STEP = {"+x": (1, 0), "-x": (-1, 0), "+z": (0, 1), "-z": (0, -1)}


def onward(message):
    colour, dx, dz, piece = message
    first = piece in ("A0", "B0", "B1")
    out = []

    def along(name, place, farthest, even):
        if place == 0:
            out.extend([("+" + name, 1), ("-" + name, -1)])
        elif 0 < place < farthest - 1 or (place == farthest - 1 and first == even):
            out.append(("+" + name, place + 1))
        elif -farthest + 1 < place < 0:
            out.append(("-" + name, place - 1))
        elif place == -farthest + 1 and first != even:
            out.append(("-" + name, farthest))

    if colour == "A":
        if dz == 0:
            along("x", dx, NX // 2, True)
            out = [(way, (colour, to, 0, piece)) for way, to in out]
            out += [("+z", (colour, dx, 1, piece)), ("-z", (colour, dx, -1, piece))]
        else:
            along("z", dz, NZ // 2, dx % 2 == 0)
            out = [(way, (colour, dx, to, piece)) for way, to in out]
    else:
        if dx == 0:
            along("z", dz, NZ // 2, True)
            out = [(way, (colour, 0, to, piece)) for way, to in out]
            out += [("+x", (colour, 1, dz, piece)), ("-x", (colour, -1, dz, piece))]
        else:
            along("x", dx, NX // 2, dz % 2 == 0)
            out = [(way, (colour, to, dz, piece)) for way, to in out]
    return out


EARLY_X = ("A0", "A1", "A2", "B0", "B3", "B1", "B2")
EARLY_Z = (("B0", "B3", "B1"), ("A0", "A1"))
EARLY = {"x": EARLY_X, "z": EARLY_Z[0] + EARLY_Z[1]}


def own_hops(pieces, axis):
    hops = [hop for piece in pieces for hop in onward((piece[0], 0, 0, piece))]
    return [(way, message) for way, message in hops if way[1] == axis]


def hops_left(message):
    hops, front = 0, [message]
    while front := [new for old in front for _, new in onward(old)]:
        hops += 1
    return hops


def plan():
    rate, latency, step, slack = 46.65e3 / 1024, 2.8, 0.05, 2.0
    stage_x, stage_z, taken_x, taken_z = 4.5, 5.5, 0.5, 1.05
    free = {way: taken_x if way[1] == "x" else 0.0 for way in STEP}
    waiting = {way: [] for way in STEP}
    events, count = [], itertools.count()

    def issue(now, way, message, width):
        free[way] = max(now, free[way]) + width * KIB[message[3]] / rate
        heapq.heappush(events, (free[way] + latency, message))

    def add(hops):
        for way, message in hops:
            heapq.heappush(waiting[way], (-hops_left(message), next(count), message))

    def sends(now):
        out = []
        for way in STEP:
            while waiting[way] and free[way] - now < slack:
                message = heapq.heappop(waiting[way])[2]
                issue(now, way, message, 1)
                out.append((way, message))
        return out

    for way, message in own_hops(EARLY_X, "x") + own_hops(EARLY_Z[0], "z"):
        issue(0.0, way, message, 2)
    now = max(stage_x, free["+z"])
    for way in ("+z", "-z"):
        free[way] = now + taken_z
    for way, message in own_hops(EARLY_Z[1], "z"):
        issue(now, way, message, 2)
    now += stage_z + 0.2
    events = [(max(at, now), message) for at, message in events]
    heapq.heapify(events)
    for axis in "xz":
        add(own_hops([p for p in PIECES if p not in EARLY[axis]], axis))
    first, steps = sends(now), []
    while events:
        at, message = heapq.heappop(events)
        now = max(now, at) + step
        add(onward(message))
        steps.append((message, sends(now)))
    return first, steps


FIRST, STEPS = plan()
INDEX = {message: i for i, (message, _) in enumerate(STEPS)}
EARLY_WAY = {message: way for axis in "xz" for way, message in own_hops(EARLY[axis], axis)}
SENT = sum(KIB[message[3]] for _, message in FIRST + [hop for _, sends in STEPS for hop in sends])


def slots():
    turn = {"+x": "-x", "-x": "+x", "+z": "-z", "-z": "+z"}
    sent = [(-1, way, message) for axis in "xz" for way, message in own_hops(EARLY[axis], axis)]
    sent += [(-1, way, message) for way, message in FIRST]
    sent += [(step, way, message) for step, (_, sends) in enumerate(STEPS) for way, message in sends]

    def known(old, way):
        later = [INDEX[m] for at, back, m in sent if back == turn[way] and at >= max(0, INDEX[old])]
        return min(later, default=len(STEPS))

    last, slot = [], {}
    for at, way, message in sorted(sent, key=lambda entry: (entry[0], INDEX[entry[2]])):
        free = [i for i, old in enumerate(last) if at >= 0 and known(old, way) <= at]
        if free:
            slot[message] = free[0]
            last[free[0]] = message
        else:
            slot[message] = len(last)
            last.append(message)
    return slot


SLOT = slots()


def gather_kernel(
    wq, fq, sq, wk, fk, sk, wv, fv, sv, nt, ns,
    oq, ok, ov, hq, hk, hv, cq, ck, cv, on,
    vq, vk, vv, vn, place, ring_n, ring_m, flat_n, part, line,
    scale, near_q, near_k, near_v, load_sem, part_recv, line_recv, norm_send, norm_recv,
    early_send, send_sem, recv_sem, pair_send, pair_recv,
):
    shard = lax.axis_index("shard")
    width = lax.axis_index("width")
    core = lax.rem(shard, NC)
    chip = lax.div(shard, NC)
    x = lax.rem(chip, NX)
    z = lax.div(chip, NX)
    other = 1 - core

    def device(zz, xx, cc):
        return (zz * NX + xx) * NC + cc

    xs = [x] + [lax.rem(x + i, NX) for i in range(1, NX)]
    zs = [z] + [lax.rem(z + i, NZ) for i in range(1, NZ)]

    loads = []
    for i, (src, dst) in enumerate(((nt, vn.at[0]), (ns, vn.at[1]))):
        loads.append(pltpu.make_async_copy(src, dst, load_sem.at[3 + i]))
    for i, src in enumerate((wq, fq, sq, wk, fk, sk, wv, fv, sv)):
        dst = (vq, vk, vv)[i // 3].at[i % 3]
        loads.append(pltpu.make_async_copy(src, dst, load_sem.at[i // 3]))
    for load in loads:
        load.start()

    x_peers = [(device(z, xs[i], c), width) for i in (2, 1, 3) for c in (other, core)]
    x_peers += [(device(z, x, other), width)]
    z_peers = [(device(zs[i], x, core), width) for i in (4, 3, 5, 2, 6, 1, 7)]
    w_peers = [(device(z, x, c), lax.rem(width + i, NW)) for i in range(1, NW) for c in (core, other)]
    barrier = pltpu.get_barrier_semaphore()
    greeted = z_peers + x_peers + w_peers
    for peer in greeted:
        pl.semaphore_signal(barrier, 1, device_id=peer, device_id_type=MESH)

    def send(src, dst, send_to, recv_at, peer):
        copy = pltpu.make_async_remote_copy(
            src_ref=src, dst_ref=dst, send_sem=send_to, recv_sem=recv_at, device_id=peer, device_id_type=MESH
        )
        copy.start()

    def await_bytes(ref, sem):
        pltpu.make_async_copy(ref, ref, sem).wait()

    def await_kib(kib, whole_q, rows_q, rows_k, sem):
        count, kib = divmod(kib, 128)
        if count:
            await_bytes(whole_q(count), sem)
        count, kib = divmod(kib, 16)
        if count:
            await_bytes(rows_q.at[pl.ds(0, 8 * count)], sem)
        count = kib // 4
        if count:
            await_bytes(rows_k.at[pl.ds(0, 8 * count)], sem)

    seat = core * NW + width
    for load in loads[:2]:
        load.wait()
    gain = (vn[0] + vn[1]).astype(jnp.bfloat16).astype(jnp.float32)
    place[...] = jnp.zeros_like(place)
    each = LANES // (NC * NW)
    for i in range(NC * NW):
        place[i : i + 1, i * each : (i + 1) * each] = gain
    ring_n[seat] = place[pl.ds(seat, 1), :]

    group = x * NC + core
    row = 0
    for n, (v, h) in enumerate(((vq, hq), (vk, hk), (vv, hv))):
        await_bytes(v, load_sem.at[n])
        for j in range(h.shape[1] // LANES):
            at = slice(j * LANES, (j + 1) * LANES)
            hold = HOLD_RATE * v[1, :, at] + v[2, :, at]
            whole = v[0, :, at] - LEARN_RATE * hold
            h[:, at] = whole
            part[group, row : row + 1, :] = jnp.sum(jnp.abs(whole), axis=0, keepdims=True)
            row += 1

    pl.semaphore_wait(barrier, len(greeted))

    ways = list(STEP)
    peers = {
        "+x": (device(z, xs[1], core), width),
        "-x": (device(z, xs[NX - 1], core), width),
        "+z": (device(zs[1], x, core), width),
        "-z": (device(zs[NZ - 1], x, core), width),
    }
    wide = (hq, hk, hv)
    near = (near_q, near_k, near_v)

    def near_ref(way, piece):
        array, start, rows = PIECES[piece]
        return near[array].at[ways.index(way), pl.ds(start, rows)]

    def early(pieces, axis):
        for way, message in own_hops(pieces, axis):
            array, start, rows = PIECES[message[3]]
            src = wide[array].at[pl.ds(start, rows)]
            send(src, near_ref(way, message[3]), early_send, recv_sem.at[SLOT[message]], peers[way])

    for peer in x_peers:
        send(part.at[group], part.at[group], norm_send, part_recv, peer)
    early(EARLY_X, "x")
    early(EARLY_Z[0], "z")
    for peer in [x_peers[-1]] + w_peers:
        send(ring_n.at[seat], ring_n.at[seat], norm_send, norm_recv.at[0], peer)
    await_bytes(part.at[pl.ds(0, 7)], part_recv)
    total = part[0]
    for i in range(1, NX * NC):
        total = total + part[i]
    line[z] = total
    for peer in z_peers:
        send(line.at[z], line.at[z], norm_send, line_recv, peer)
    early(EARLY_Z[1], "z")

    await_bytes(line.at[pl.ds(0, 7)], line_recv)
    total = line[0]
    for i in range(1, NZ):
        total = total + line[i]
    column = total * (1.0 / D_MODEL)
    cq[...] = column[0:8]
    ck[...] = column[8:10]
    cv[...] = column[10:12]
    scale[...] = 1.0 / column

    outs = (oq, ok, ov)
    pair = (device(z, x, other), width)

    def block(dx, dz):
        return zs[-dz % NZ] * NX + xs[-dx % NX]

    def piece_ref(dx, dz, piece):
        array, start, rows = PIECES[piece]
        return outs[array].at[block(dx, dz), core, pl.ds(start, rows)]

    def forward(way, message):
        _, dx, dz, piece = message
        ref = piece_ref(dx - STEP[way][0], dz - STEP[way][1], piece)
        send(ref, ref, send_sem, recv_sem.at[SLOT[message]], peers[way])

    def across(dx, dz, piece):
        ref = piece_ref(dx, dz, piece)
        array = PIECES[piece][0]
        send(ref, ref, pair_send.at[array], pair_recv.at[array], pair)

    def narrow(src, to, piece):
        array, start, rows = PIECES[piece]
        row = sum(h.shape[1] for h in wide[:array]) // LANES
        for j in range(wide[array].shape[1] // LANES):
            at = slice(j * LANES, (j + 1) * LANES)
            part_of = src[:, at] * scale[row + j : row + j + 1, :]
            outs[array][to, core, start : start + rows, at] = part_of.astype(jnp.bfloat16)

    for piece, (array, start, rows) in PIECES.items():
        narrow(wide[array].at[pl.ds(start, rows)], chip, piece)
    for way, message in FIRST:
        forward(way, message)
    for piece in PIECES:
        across(0, 0, piece)
    for step, (message, sends) in enumerate(STEPS):
        _, dx, dz, piece = message
        if message in EARLY_WAY:
            src = near_ref(EARLY_WAY[message], piece)
            await_bytes(src, recv_sem.at[SLOT[message]])
            narrow(src, block(dx, dz), piece)
        else:
            await_bytes(piece_ref(dx, dz, piece), recv_sem.at[SLOT[message]])
        for way, new in sends:
            forward(way, new)
        across(dx, dz, piece)
        if step == len(STEPS) // 4:
            await_bytes(ring_n.at[pl.ds(0, 7)], norm_recv.at[0])
            gain = ring_n[0]
            for i in range(1, NC * NW):
                gain = gain + ring_n[i]
            ring_m[z, x] = gain
            for i in range(1, NX):
                peer = (device(z, xs[i], core), width)
                send(ring_m.at[z, x], ring_m.at[z, x], norm_send, norm_recv.at[1], peer)
        if step == len(STEPS) // 2:
            await_bytes(ring_m.at[0, pl.ds(0, 3)], norm_recv.at[1])
            for peer in z_peers:
                send(ring_m.at[z], ring_m.at[z], norm_send, norm_recv.at[2], peer)

    await_bytes(ring_m.at[pl.ds(0, 7)], norm_recv.at[2])
    for i in range(NZ * NX):
        flat_n[i : i + 1, :] = ring_m[i // NX, i % NX]
    on[...] = flat_n[...].astype(jnp.bfloat16)

    for i, out in enumerate(outs):
        await_bytes(out.at[:, other], pair_recv.at[i])
        await_bytes(out.at[:, core], pair_send.at[i])
    half = SENT // 8 * 4
    for kib in (half, SENT - half):
        await_kib(kib, lambda n: oq.at[pl.ds(0, n), 0], oq.at[0, 0], ok.at[0, 0], send_sem)
    early_kib = 2 * sum(KIB[p] for axis in "xz" for p in EARLY[axis])
    for _ in range(2):
        await_kib(early_kib // 2, lambda n: near_q.at[pl.ds(0, n)], hq, hk, early_send)
    await_bytes(part.at[pl.ds(0, 7)], norm_send)
    await_bytes(line.at[pl.ds(0, 7)], norm_send)
    await_bytes(ring_n.at[pl.ds(0, 7)], norm_send)
    await_bytes(ring_m.at[0, pl.ds(0, 3)], norm_send)
    await_bytes(ring_m.at[pl.ds(0, 7)], norm_send)


def write_kernel(*refs):
    count = (len(refs) - 1) // 2
    copies = [pltpu.make_async_copy(refs[i], refs[count + i], refs[-1].at[i]) for i in range(count)]
    for copy in copies:
        copy.start()
    for copy in copies:
        copy.wait()


def local(wq, fq, sq, wk, fk, sk, wv, fv, sv, nt, ns):
    q, k, v = wq.shape[1], wk.shape[1], wv.shape[1]
    cols = (q, k, v)
    tiles = sum(cols) // LANES
    f32, bf16 = jnp.float32, jnp.bfloat16
    shapes = [((NZ * NX, NC, ROWS, n), bf16) for n in cols]
    shapes += [((ROWS, n), f32) for n in cols]
    shapes += [((n // LANES, LANES), f32) for n in cols]
    shapes += [((NZ * NX, LANES), bf16)]
    args = (wq, fq, sq, wk, fk, sk, wv, fv, sv, nt.reshape(1, -1), ns.reshape(1, -1))
    gathered = pl.pallas_call(
        gather_kernel,
        out_shape=[pltpu.VMEM(*s) for s in shapes],
        in_specs=[pl.BlockSpec(memory_space=pltpu.HBM)] * 11,
        out_specs=[pl.BlockSpec(memory_space=pltpu.VMEM)] * len(shapes),
        scratch_shapes=[
            pltpu.VMEM((3, ROWS, q), f32),
            pltpu.VMEM((3, ROWS, k), f32),
            pltpu.VMEM((3, ROWS, v), f32),
            pltpu.VMEM((2, 1, LANES // (NC * NW)), f32),
            pltpu.VMEM((NC * NW, LANES), f32),
            pltpu.VMEM((NC * NW, 1, LANES), f32),
            pltpu.VMEM((NZ, NX, 1, LANES), f32),
            pltpu.VMEM((NZ * NX, LANES), f32),
            pltpu.VMEM((NX * NC, tiles, LANES), f32),
            pltpu.VMEM((NZ, tiles, LANES), f32),
            pltpu.VMEM((tiles, LANES), f32),
            pltpu.VMEM((4, ROWS, q), f32),
            pltpu.VMEM((4, ROWS, k), f32),
            pltpu.VMEM((4, ROWS, v), f32),
            pltpu.SemaphoreType.DMA((5,)),
            pltpu.SemaphoreType.DMA,
            pltpu.SemaphoreType.DMA,
            pltpu.SemaphoreType.DMA,
            pltpu.SemaphoreType.DMA((3,)),
            pltpu.SemaphoreType.DMA,
            pltpu.SemaphoreType.DMA,
            pltpu.SemaphoreType.DMA((1 + max(SLOT.values()),)),
            pltpu.SemaphoreType.DMA((3,)),
            pltpu.SemaphoreType.DMA((3,)),
        ],
        compiler_params=pltpu.CompilerParams(
            collective_id=0, has_side_effects=True, vmem_limit_bytes=40 * 1024 * 1024
        ),
        name="update_sum_gather",
    )(*(pltpu.with_memory_space_constraint(a, pltpu.HBM) for a in args))
    written = pl.pallas_call(
        write_kernel,
        out_shape=[jax.ShapeDtypeStruct(*s) for s in shapes],
        in_specs=[pl.BlockSpec(memory_space=pltpu.VMEM)] * len(shapes),
        out_specs=[pl.BlockSpec(memory_space=pltpu.HBM)] * len(shapes),
        scratch_shapes=[pltpu.SemaphoreType.DMA((len(shapes),))],
        compiler_params=pltpu.CompilerParams(vmem_limit_bytes=1024 * 1024),
        name="write_outputs",
    )(*gathered)
    oq, ok, ov, hq, hk, hv, cq, ck, cv, on = written
    return (
        oq.reshape(D_MODEL, q),
        ok.reshape(D_MODEL, k),
        ov.reshape(D_MODEL, v),
        cq.reshape(q),
        ck.reshape(k),
        cv.reshape(v),
        on.reshape(D_MODEL),
        hq,
        hk,
        hv,
    )


def solution(mesh):
    block = P("shard", "width")
    spread = P(("shard", "width"))
    return jax.shard_map(
        local,
        mesh=mesh,
        in_specs=(block,) * 9 + (spread, spread),
        out_specs=(P(None, "width"),) * 3 + (P("width"),) * 3 + (P(),) + (block,) * 3,
        check_vma=False,
    )
```
